32 devices in a mesh: shard: 4 (over y, x), context: 4 (over z), tensor: 2 (over core).
Axes of the slice: x: 2, y: 2, z: 4, core: 2. Of those that a mesh axis runs over, the one named last changes fastest.
Arguments:
- hidden_in: bfloat16 [8, 1024, 2048], P('shard', 'context'), may hold values from -6 to 6
- cotangent: bfloat16 [8, 1024, 2048], P('shard', 'context'), may hold values from -6 to 6
- seq_lengths: int32 [8], P('shard'), may hold values from 256 to 1024, as said below
- adapter_ids: int32 [8], P('shard'), may hold values from 0 to 7
- attn_gain: bfloat16 [2048], replicated, may hold values from 0.25 to 1.75
- ffn_gain: bfloat16 [2048], replicated, may hold values from 0.25 to 1.75
- query_weight: bfloat16 [2048, 2048], P(('shard', 'context'), 'tensor'), may hold values from -0.125 to 0.125
- key_weight: bfloat16 [2048, 1024], P(('shard', 'context'), 'tensor'), may hold values from -0.125 to 0.125
- value_weight: bfloat16 [2048, 1024], P(('shard', 'context'), 'tensor'), may hold values from -0.125 to 0.125
- output_weight: bfloat16 [2048, 2048], P(('shard', 'context'), 'tensor'), may hold values from -0.5 to 0.5
- gate_weight: bfloat16 [2048, 8192], P(('shard', 'context'), 'tensor'), may hold values from -0.125 to 0.125
- up_weight: bfloat16 [2048, 8192], P(('shard', 'context'), 'tensor'), may hold values from -0.125 to 0.125
- down_weight: bfloat16 [2048, 8192], P(('shard', 'context'), 'tensor'), may hold values from -0.0625 to 0.0625
- qkv_entry: bfloat16 [2048, 128], P(('shard', 'context')), may hold values from -0.125 to 0.125
- query_exit: bfloat16 [128, 2048], P(('shard', 'context'), 'tensor'), may hold values from -1.5 to 1.5
- key_exit: bfloat16 [128, 1024], P(('shard', 'context'), 'tensor'), may hold values from -1.5 to 1.5
- value_exit: bfloat16 [128, 1024], P(('shard', 'context'), 'tensor'), may hold values from -1.5 to 1.5
- attn_entry: bfloat16 [128, 2048], P(('shard', 'context'), 'tensor'), may hold values from -0.5 to 0.5
- attn_exit: bfloat16 [2048, 128], P(('shard', 'context')), may hold values from -1.5 to 1.5
- gate_entry: bfloat16 [2048, 128], P(('shard', 'context')), may hold values from -0.125 to 0.125
- gate_exit: bfloat16 [128, 8192], P(('shard', 'context'), 'tensor'), may hold values from -1.5 to 1.5
- up_entry: bfloat16 [2048, 128], P(('shard', 'context')), may hold values from -0.125 to 0.125
- up_exit: bfloat16 [128, 8192], P(('shard', 'context'), 'tensor'), may hold values from -1.5 to 1.5
- down_entry: bfloat16 [128, 8192], P(('shard', 'context'), 'tensor'), may hold values from -0.0625 to 0.0625
- down_exit: bfloat16 [2048, 128], P(('shard', 'context')), may hold values from -1.5 to 1.5
Outputs:
- layer_out: bfloat16 [8, 1024, 2048], P('shard', 'context')
- input_grad: bfloat16 [8, 1024, 2048], P('shard', 'context')
- qkv_entry_grad: float32 [2048, 128], P(('shard', 'context'))
- query_exit_grad: float32 [128, 2048], P(('shard', 'context'), 'tensor')
- key_exit_grad: float32 [128, 1024], P(('shard', 'context'), 'tensor')
- value_exit_grad: float32 [128, 1024], P(('shard', 'context'), 'tensor')
- attn_entry_grad: float32 [128, 2048], P(('shard', 'context'), 'tensor')
- attn_exit_grad: float32 [2048, 128], P(('shard', 'context'))
- gate_entry_grad: float32 [2048, 128], P(('shard', 'context'))
- gate_exit_grad: float32 [128, 8192], P(('shard', 'context'), 'tensor')
- up_entry_grad: float32 [2048, 128], P(('shard', 'context'))
- up_exit_grad: float32 [128, 8192], P(('shard', 'context'), 'tensor')
- down_entry_grad: float32 [128, 8192], P(('shard', 'context'), 'tensor')
- down_exit_grad: float32 [2048, 128], P(('shard', 'context'))
The draws below stay inside these ranges and needn't reach their ends.
Inputs may be any that keep to these rules, and one draw needn't show every extreme that they name: Each sequence's valid positions are the first seq_lengths of its slot; in every draw some sequence fills its whole slot of 1024 and some has exactly 256.
All inputs are finite; a program needn't handle non-finite values.
Results may differ from the reference program's by a relative error of at most 0.019.
Values may be sent and summed in bfloat16 or wider, within the bound.
A program may use at most 320 MiB of HBM per device.

```python
import math
import jax
import jax.numpy as jnp
from jax import lax

D = 2048
QH = 16
KVH = 8
HD = 128
FF = 8192
ADAPTERS = 8
RANK = 16
LEN = 1024
SEQ_GRP = 2
SEQS = 8
AR = 128
N_SHARD = 4


def draw_seq_lengths(key, part):
    first, second, third = jax.random.split(key, 3)
    drawn = jax.random.randint(first, (SEQS,), LEN // 4, LEN + 1)
    full_at = jax.random.randint(second, (), 0, SEQS)
    short_at = (full_at + 1 + jax.random.randint(third, (), 0, SEQS - 1)) % SEQS
    indices = jnp.arange(SEQS)
    drawn = jnp.where(indices == full_at, LEN, drawn)
    drawn = jnp.where(indices == short_at, LEN // 4, drawn)
    return drawn.astype(jnp.int32)


def with_ends(values, rng, smallest, top_value):
    longest = values.shape.index(max(values.shape))
    spots = []
    for shift in (0, 1):
        where = [jax.random.randint(jax.random.fold_in(rng, axis), (), 0, length) for axis, length in enumerate(values.shape)]
        where[longest] = (where[longest] + shift) % values.shape[longest]
        spots.append(tuple(where))
    return values.at[spots[0]].set(smallest).at[spots[1]].set(top_value)


def shard_levels(stream_key, shape, cuts, low, high):
    level, own = 1.0, jax.random.fold_in(stream_key, 6)
    for position, shards_of in cuts:
        draws = jnp.exp(jax.random.uniform(jax.random.fold_in(own, position), (shards_of,), jnp.float32, low / len(cuts), high / len(cuts)))
        level = level * jnp.repeat(draws, shape[position] // shards_of).reshape([-1 if axis == position else 1 for axis in range(len(shape))])
    return level


def centred(own_key, extent, width, limit, shards=(), kind=jnp.bfloat16):
    array = jax.random.normal(own_key, extent, jnp.float32) * width
    if len(shards) > 0:
        array = shard_levels(own_key, extent, shards, -0.22, 0.18) * array
    return jnp.clip(array, min=-limit, max=limit).astype(kind)


def setup_inputs(seed: int = 0) -> dict:
    key_of = jax.random.split(jax.random.key(seed), 26)
    return {
        "hidden_in": centred(key_of[0], (SEQS, LEN, D), 1.0, 6.0, ((0, 4), (1, 4))),
        "cotangent": centred(key_of[1], (SEQS, LEN, D), 1.0, 6.0, ((0, 4), (1, 4))),
        "seq_lengths": draw_seq_lengths(jax.random.fold_in(key_of[25], 71), 0),
        "adapter_ids": with_ends(jax.random.randint(key_of[3], (SEQS,), 0, ADAPTERS), jax.random.fold_in(key_of[3], 1), 0, ADAPTERS - 1).astype(jnp.int32),
        "attn_gain": jnp.clip(1.0 + 0.15 * jax.random.normal(key_of[4], (D,), jnp.float32), 0.25, 1.75).astype(jnp.bfloat16),
        "ffn_gain": jnp.clip(1.0 + 0.15 * jax.random.normal(key_of[5], (D,), jnp.float32), 0.25, 1.75).astype(jnp.bfloat16),
        "query_weight": centred(key_of[6], (D, QH * HD), D ** -0.5, 0.125, ((0, 16), (1, 2))),
        "key_weight": centred(key_of[7], (D, KVH * HD), D ** -0.5, 0.125, ((0, 16), (1, 2))),
        "value_weight": centred(key_of[8], (D, KVH * HD), D ** -0.5, 0.125, ((0, 16), (1, 2))),
        "output_weight": centred(key_of[9], (D, QH * HD), (QH * HD // 16) ** -0.5, 0.5, ((0, 16), (1, 2))),
        "gate_weight": centred(key_of[10], (D, FF), D ** -0.5, 0.125, ((0, 16), (1, 2))),
        "up_weight": centred(key_of[11], (D, FF), D ** -0.5, 0.125, ((0, 16), (1, 2))),
        "down_weight": centred(key_of[12], (D, FF), FF ** -0.5, 0.0625, ((0, 16), (1, 2))),
        "qkv_entry": centred(key_of[13], (D, AR), D ** -0.5, 0.125, ((0, 16),)),
        "query_exit": centred(key_of[14], (AR, QH * HD), RANK ** -0.5, 1.5, ((0, 16), (1, 2))),
        "key_exit": centred(key_of[15], (AR, KVH * HD), RANK ** -0.5, 1.5, ((0, 16), (1, 2))),
        "value_exit": centred(key_of[16], (AR, KVH * HD), RANK ** -0.5, 1.5, ((0, 16), (1, 2))),
        "attn_entry": centred(key_of[17], (AR, QH * HD), (QH * HD // 16) ** -0.5, 0.5, ((0, 16), (1, 2))),
        "attn_exit": centred(key_of[18], (D, AR), RANK ** -0.5, 1.5, ((0, 16),)),
        "gate_entry": centred(key_of[19], (D, AR), D ** -0.5, 0.125, ((0, 16),)),
        "gate_exit": centred(key_of[20], (AR, FF), RANK ** -0.5, 1.5, ((0, 16), (1, 2))),
        "up_entry": centred(key_of[21], (D, AR), D ** -0.5, 0.125, ((0, 16),)),
        "up_exit": centred(key_of[22], (AR, FF), RANK ** -0.5, 1.5, ((0, 16), (1, 2))),
        "down_entry": centred(key_of[23], (AR, FF), FF ** -0.5, 0.0625, ((0, 16), (1, 2))),
        "down_exit": centred(key_of[24], (D, AR), RANK ** -0.5, 1.5, ((0, 16),)),
    }


EPSILON = 1e-05
ROPE_BASE = 1000000.0
MASKED = -1e+30
HIGHEST = lax.Precision.HIGHEST

@jax.custom_vjp
def low(v):
    return lax.optimization_barrier(v.astype(jnp.bfloat16)).astype(jnp.float32)

@jax.custom_vjp
def low_back(v):
    return v

def low_keep(v):
    return (low(v), None)

def low_pass(kept, grad):
    return (grad,)

def back_keep(v):
    return (v, None)

def back_low(kept, grad):
    return (low(grad),)
low.defvjp(low_keep, low_pass)
low_back.defvjp(back_keep, back_low)

def product(left, right):
    return jnp.dot(left, right, precision=HIGHEST, preferred_element_type=jnp.float32)

def rms_scale(values, gain):
    return values * lax.rsqrt(lax.optimization_barrier(jnp.mean(values * values, axis=-1, keepdims=True)) + EPSILON) * gain

def rotate(values, positions):
    half_width = values.shape[-1] // 2
    inverse = ROPE_BASE ** (-2.0 * jnp.arange(half_width).astype(jnp.float32) / values.shape[-1])
    angles = positions.astype(jnp.float32)[:, None] * inverse[None, :]
    cosine = jnp.cos(angles)[:, None, :]
    sine = jnp.sin(angles)[:, None, :]
    first = values[..., :half_width]
    second = values[..., half_width:]
    return jnp.concatenate([first * cosine - second * sine, second * cosine + first * sine], axis=-1)

def attend(queries, key_heads, value_heads, lengths):
    groups = queries.shape[0]
    seq_len = queries.shape[1]
    block = min(512, seq_len)
    repeat = QH // KVH
    scale = 1.0 / math.sqrt(HD)
    key_positions = jnp.arange(seq_len).astype(jnp.int32)

    def one_block(offset):
        rows = lax.dynamic_slice_in_dim(queries, offset, block, 1).reshape(groups, block, KVH, repeat, HD)
        scores = jnp.einsum('gqcrd,gkcd->gcrqk', rows, key_heads, precision=HIGHEST) * scale
        scores = low_back(scores)
        query_positions = offset + jnp.arange(block).astype(jnp.int32)
        allowed = (key_positions[None, None, :] <= query_positions[None, :, None]) & (key_positions[None, None, :] < lengths[:, None, None])
        scores = jnp.where(allowed[:, None, None], scores, MASKED)
        weights = low(jax.nn.softmax(scores, axis=-1))
        mixed = jnp.einsum('gcrqk,gkcd->gqcrd', weights, value_heads, precision=HIGHEST)
        return mixed.reshape(groups, block, QH * HD)
    offsets = (jnp.arange(seq_len // block) * block).astype(jnp.int32)
    blocks = lax.map(jax.checkpoint(one_block), offsets)
    return jnp.moveaxis(blocks, 0, 1).reshape(groups, seq_len, QH * HD)

def layer_forward(inputs, lengths, adapter_rows, adapters, frozen):
    attn_gain, ffn_gain, query_weight, key_weight, value_weight, output_weight, gate_weight, up_weight, down_weight = frozen
    qkv_entry, query_exit, key_exit, value_exit, attn_entry, attn_exit, gate_entry, gate_exit, up_entry, up_exit, down_entry, down_exit = adapters
    groups = inputs.shape[0]
    seq_len = inputs.shape[1]
    positions = jnp.arange(seq_len).astype(jnp.int32)
    valid = (positions[None, :] < lengths[:, None]).astype(jnp.float32)[:, :, None]
    select = (jnp.arange(ADAPTERS * RANK).astype(jnp.int32)[None, :] // RANK == adapter_rows[:, None]).astype(jnp.float32)[:, None, :]
    normed_one = low(rms_scale(inputs, attn_gain))
    entry_qkv = low(low_back(select * product(normed_one, qkv_entry)))
    query_raw = low_back(product(normed_one, query_weight) + product(entry_qkv, query_exit))
    key_raw = low_back(product(normed_one, key_weight) + product(entry_qkv, key_exit))
    value_raw = low_back(product(normed_one, value_weight) + product(entry_qkv, value_exit))
    query_rot = low(rotate(query_raw.reshape(groups, seq_len, QH, HD), positions))
    key_rot = low(rotate(key_raw.reshape(groups, seq_len, KVH, HD), positions))
    value_low = low(value_raw.reshape(groups, seq_len, KVH, HD))
    attended = low(low_back(attend(query_rot, key_rot, value_low, lengths)))
    entry_attn = low(low_back(select * product(attended, attn_entry.T)))
    mid = inputs + low_back(product(attended, output_weight.T) + product(entry_attn, attn_exit.T))
    normed_two = low(rms_scale(mid, ffn_gain))
    entry_gate = low(low_back(select * product(normed_two, gate_entry)))
    entry_up = low(low_back(select * product(normed_two, up_entry)))
    gate_pre = low_back(product(normed_two, gate_weight) + product(entry_gate, gate_exit))
    up_pre = low_back(product(normed_two, up_weight) + product(entry_up, up_exit))
    hidden_low = low(jax.nn.silu(gate_pre) * up_pre)
    entry_down = low(low_back(select * product(hidden_low, down_entry.T)))
    branch = low_back(product(hidden_low, down_weight.T) + product(entry_down, down_exit.T))
    return valid * (mid + branch)

def reference(hidden_in, cotangent, seq_lengths, adapter_ids, attn_gain, ffn_gain, query_weight, key_weight, value_weight, output_weight, gate_weight, up_weight, down_weight, qkv_entry, query_exit, key_exit, value_exit, attn_entry, attn_exit, gate_entry, gate_exit, up_entry, up_exit, down_entry, down_exit):
    frozen = tuple((item.astype(jnp.float32) for item in (attn_gain, ffn_gain, query_weight, key_weight, value_weight, output_weight, gate_weight, up_weight, down_weight)))
    adapters = tuple((item.astype(jnp.float32) for item in (qkv_entry, query_exit, key_exit, value_exit, attn_entry, attn_exit, gate_entry, gate_exit, up_entry, up_exit, down_entry, down_exit)))
    inputs_all = hidden_in.astype(jnp.float32).reshape(N_SHARD, SEQ_GRP, LEN, D)
    cotan_all = cotangent.astype(jnp.float32).reshape(N_SHARD, SEQ_GRP, LEN, D)
    lengths_all = seq_lengths.astype(jnp.int32).reshape(N_SHARD, SEQ_GRP)
    chosen_all = adapter_ids.astype(jnp.int32).reshape(N_SHARD, SEQ_GRP)

    def group_step(running, packed):
        inputs, cotan, lengths, chosen = packed
        result, pullback = jax.vjp(lambda values, weights: layer_forward(values, lengths, chosen, weights, frozen), inputs, adapters)
        input_part, adapter_part = pullback(cotan)
        running = tuple((first + second for first, second in zip(running, adapter_part)))
        return (running, (result, input_part))
    initial = tuple((jnp.zeros_like(item) for item in adapters))
    totals, (results, input_parts) = lax.scan(group_step, initial, (inputs_all, cotan_all, lengths_all, chosen_all))
    layer_out = results.reshape(SEQS, LEN, D).astype(jnp.bfloat16)
    input_grad = input_parts.reshape(SEQS, LEN, D).astype(jnp.bfloat16)
    return (layer_out, input_grad, totals[0], totals[1], totals[2], totals[3], totals[4], totals[5], totals[6], totals[7], totals[8], totals[9], totals[10], totals[11])
```

```python
import math

import jax
import jax.numpy as jnp
from jax import lax
from jax.sharding import PartitionSpec as P

HD = 128
RANK = 16
EPSILON = 1e-05
ROPE_BASE = 1000000.0
MASKED = -1e30
F32 = jnp.float32
BF16 = jnp.bfloat16
PLANE = ("tensor", "shard")


def dot(left, right):
    return jnp.dot(left, right, preferred_element_type=F32)


def dot_t(left, right):
    return lax.dot_general(left, right, (((1,), (1,)), ((), ())), preferred_element_type=F32)


def token_sum(left, right):
    return lax.dot_general(left, right, (((0,), (0,)), ((), ())), preferred_element_type=F32)


def rms_scale(values, gain):
    return values * lax.rsqrt(jnp.mean(values * values, axis=-1, keepdims=True) + EPSILON) * gain


def norm_back(values, gain, grad):
    r = lax.rsqrt(jnp.mean(values * values, axis=-1, keepdims=True) + EPSILON)
    scaled = grad * gain
    return r * scaled - values * (r * r * r * jnp.mean(values * scaled, axis=-1, keepdims=True))


def rope_tables(length):
    half = HD // 2
    inverse = ROPE_BASE ** (-2.0 * jnp.arange(half).astype(F32) / HD)
    angles = jnp.arange(length).astype(F32)[:, None] * inverse[None, :]
    return jnp.cos(angles), jnp.sin(angles)


def rotate(values, cosine, sine):
    half = HD // 2
    first, second = values[..., :half], values[..., half:]
    return jnp.concatenate(
        [first * cosine - second * sine, second * cosine + first * sine], axis=-1
    )


def gather_tokens(values):
    return lax.all_gather(values, PLANE, axis=0, tiled=True)


def scatter_tokens(values):
    return lax.psum_scatter(
        values.astype(BF16), PLANE, scatter_dimension=0, tiled=True
    ).astype(F32)


def shards(
    hidden_in,
    cotangent,
    seq_lengths,
    adapter_ids,
    attn_gain,
    ffn_gain,
    query_weight,
    key_weight,
    value_weight,
    output_weight,
    gate_weight,
    up_weight,
    down_weight,
    qkv_entry,
    query_exit,
    key_exit,
    value_exit,
    attn_entry,
    attn_exit,
    gate_entry,
    gate_exit,
    up_entry,
    up_exit,
    down_entry,
    down_exit,
):
    n_s, n_c = lax.axis_size("shard"), lax.axis_size("context")
    s, t = lax.axis_index("shard"), lax.axis_index("tensor")
    groups, local_len, width = hidden_in.shape
    block = width // (n_s * n_c)
    full_len = local_len * n_c
    tokens = groups * full_len
    ranks = qkv_entry.shape[1]
    swap = [(a * n_c + b, b * n_c + a) for a in range(n_s) for b in range(n_c)]

    def to_layer(values):
        own = lax.dynamic_index_in_dim(values, t, 0, keepdims=False)
        own = own.reshape(local_len, n_s, n_c, block).transpose(0, 2, 1, 3)
        return lax.ppermute(own.reshape(local_len, width), ("shard", "context"), swap)

    def from_layer(values):
        own = values.reshape(local_len, n_c, n_s, block).transpose(0, 2, 1, 3)
        own = lax.ppermute(own.reshape(local_len, width), ("shard", "context"), swap)
        return lax.all_gather(own, "tensor", axis=0)

    def features(vector):
        return vector.reshape(n_s, n_c, block).transpose(1, 0, 2).reshape(width).astype(F32)

    def split(weights):
        rows, cols = weights.shape
        return weights.reshape(rows, n_s, cols // n_s).transpose(1, 0, 2)

    kv_heads_here = key_weight.shape[1] // HD
    kv_take = max(1, kv_heads_here // n_s)
    kv_first = [q * kv_heads_here // n_s for q in range(n_s)]

    def split_kv(weights):
        return jnp.stack([weights[:, h * HD : (h + kv_take) * HD] for h in kv_first])

    x_low = to_layer(hidden_in)
    cot_low = to_layer(cotangent)
    lengths, ids = lax.ppermute(
        jnp.stack([seq_lengths, adapter_ids]), ("shard", "context"), swap
    )
    gain_one, gain_two = features(attn_gain), features(ffn_gain)
    positions = s * local_len + jnp.arange(local_len)
    valid = (positions < lengths[t]).astype(F32)[:, None]
    chosen = (jnp.arange(ranks)[None, :] // RANK == ids[:, None]).astype(F32)
    select_own = chosen[t][None, :]
    select_all = jnp.broadcast_to(chosen[:, None, :], (groups, full_len, ranks)).reshape(
        tokens, ranks
    )

    def spread(pieces):
        swapped = lax.all_to_all(pieces, "shard", 0, 0, tiled=True)
        return lax.all_gather(swapped, "context", axis=0)

    attn_w = spread(
        jnp.concatenate(
            [split(query_weight), split_kv(key_weight), split_kv(value_weight), split(output_weight)],
            axis=2,
        )
    ).reshape(width, -1)
    attn_e = (
        spread(
            jnp.concatenate(
                [split(query_exit), split_kv(key_exit), split_kv(value_exit), split(attn_entry)],
                axis=2,
            )
        )
        .transpose(1, 0, 2, 3)
        .reshape(ranks, -1)
    )
    ffn_w = spread(
        jnp.concatenate([split(gate_weight), split(up_weight), split(down_weight)], axis=2)
    ).reshape(width, -1)
    ffn_e = (
        spread(jnp.concatenate([split(gate_exit), split(up_exit), split(down_entry)], axis=2))
        .transpose(1, 0, 2, 3)
        .reshape(ranks, -1)
    )
    entries = lax.all_gather(
        jnp.concatenate([qkv_entry, attn_exit, gate_entry, up_entry, down_exit], axis=1),
        ("context", "shard"),
        axis=0,
        tiled=True,
    )
    qkv_in, attn_out, gate_in, up_in, down_out = (
        entries[:, i * ranks : (i + 1) * ranks] for i in range(5)
    )
    q_cols = query_weight.shape[1] // n_s
    k_cols = kv_take * HD
    f_cols = gate_weight.shape[1] // n_s
    w_qkv, w_o = attn_w[:, : q_cols + 2 * k_cols], attn_w[:, q_cols + 2 * k_cols :]
    e_qkv, e_o = attn_e[:, : q_cols + 2 * k_cols], attn_e[:, q_cols + 2 * k_cols :]
    w_g, w_u, w_d = (ffn_w[:, i * f_cols : (i + 1) * f_cols] for i in range(3))
    e_g, e_u, e_d = (ffn_e[:, i * f_cols : (i + 1) * f_cols] for i in range(3))

    inputs = x_low.astype(F32)
    n1 = gather_tokens(rms_scale(inputs, gain_one).astype(BF16))
    en_qkv = (select_all * dot(n1, qkv_in)).astype(BF16)
    qkv = dot(n1, w_qkv) + dot(en_qkv, e_qkv)
    heads = q_cols // HD
    repeat = heads // kv_take
    cosine, sine = rope_tables(full_len)
    cos_h, sin_h = cosine[None, :, None, :], sine[None, :, None, :]
    query = rotate(qkv[:, :q_cols].reshape(groups, full_len, heads, HD), cos_h, sin_h)
    query = query.astype(BF16).reshape(groups, full_len, kv_take, repeat, HD)
    key = rotate(
        qkv[:, q_cols : q_cols + k_cols].reshape(groups, full_len, kv_take, HD), cos_h, sin_h
    ).astype(BF16)
    value = qkv[:, q_cols + k_cols :].astype(BF16).reshape(groups, full_len, kv_take, HD)
    scale = 1.0 / math.sqrt(HD)
    at = jnp.arange(full_len)
    allowed = (at[None, None, :] <= at[None, :, None]) & (at[None, None, :] < lengths[:, None, None])
    allowed = allowed[:, None, None]
    scores = jnp.einsum("gqcrd,gkcd->gcrqk", query, key, preferred_element_type=F32) * scale
    scores = jnp.where(allowed, scores, MASKED)
    largest = jnp.max(scores, axis=-1, keepdims=True)
    exponent = jnp.exp(scores - largest)
    totals = jnp.sum(exponent, axis=-1, keepdims=True)
    probs = exponent / totals
    attended = jnp.einsum(
        "gcrqk,gkcd->gqcrd", probs.astype(BF16), value, preferred_element_type=F32
    )
    att = attended.reshape(tokens, q_cols).astype(BF16)
    total = scatter_tokens(jnp.concatenate([dot_t(att, w_o), dot_t(att, e_o)], axis=1))
    en_attn = (select_own * total[:, width:]).astype(BF16)
    mid = inputs + total[:, :width] + dot_t(en_attn, attn_out)

    n2_own = rms_scale(mid, gain_two).astype(BF16)
    both = gather_tokens(jnp.concatenate([n2_own, en_attn], axis=1))
    n2, en_attn_all = both[:, :width], both[:, width:]
    en_gate = (select_all * dot(n2, gate_in)).astype(BF16)
    en_up = (select_all * dot(n2, up_in)).astype(BF16)
    gate = dot(n2, w_g) + dot(en_gate, e_g)
    up = dot(n2, w_u) + dot(en_up, e_u)
    sig = jax.nn.sigmoid(gate)
    hidden = (gate * sig * up).astype(BF16)
    total = scatter_tokens(jnp.concatenate([dot_t(hidden, w_d), dot_t(hidden, e_d)], axis=1))
    en_down = (select_own * total[:, width:]).astype(BF16)
    layer_sum = mid + total[:, :width] + dot_t(en_down, down_out)
    layer_out = from_layer((valid * layer_sum).astype(BF16))

    grad_out = valid * cot_low.astype(F32)
    g_low = gather_tokens(grad_out.astype(BF16))
    g_en_down = (select_all * dot(g_low, down_out)).astype(BF16)
    down_entry_grad = token_sum(g_en_down, hidden)
    g_hidden = dot(g_low, w_d) + dot(g_en_down, e_d)
    g_gate = (g_hidden * up * (sig * (1.0 + gate * (1.0 - sig)))).astype(BF16)
    g_up = (g_hidden * gate * sig).astype(BF16)
    gate_exit_grad = token_sum(en_gate, g_gate)
    up_exit_grad = token_sum(en_up, g_up)
    total = scatter_tokens(
        jnp.concatenate(
            [dot_t(g_gate, w_g) + dot_t(g_up, w_u), dot_t(g_gate, e_g), dot_t(g_up, e_u)], axis=1
        )
    )
    g_en_gate = (select_own * total[:, width : width + ranks]).astype(BF16)
    g_en_up = (select_own * total[:, width + ranks :]).astype(BF16)
    g_two = total[:, :width] + dot_t(g_en_gate, gate_in) + dot_t(g_en_up, up_in)
    g_mid = grad_out + norm_back(mid, gain_two, g_two)
    both = gather_tokens(
        jnp.concatenate([g_mid.astype(BF16), g_en_gate, g_en_up, en_down], axis=1)
    )
    g_mid_all = both[:, :width]
    g_en_gate_all, g_en_up_all, en_down_all = (
        both[:, width + i * ranks : width + (i + 1) * ranks] for i in range(3)
    )

    def rows_of(values):
        mine = lax.dynamic_index_in_dim(
            values.reshape(tokens, n_c, n_s, block), s, 2, keepdims=False
        )
        return mine.reshape(tokens, n_c * block)

    n2_rows = rows_of(n2)
    gate_entry_grad = token_sum(n2_rows, g_en_gate_all)
    up_entry_grad = token_sum(n2_rows, g_en_up_all)
    down_exit_grad = token_sum(rows_of(g_low), en_down_all)
    attn_exit_grad = token_sum(rows_of(g_mid_all), en_attn_all)

    g_en_attn = (select_all * dot(g_mid_all, attn_out)).astype(BF16)
    attn_entry_grad = token_sum(g_en_attn, att)
    g_att = (dot(g_mid_all, w_o) + dot(g_en_attn, e_o)).astype(BF16)
    g_heads = g_att.reshape(groups, full_len, kv_take, repeat, HD)
    g_probs = jnp.einsum("gqcrd,gkcd->gcrqk", g_heads, value, preferred_element_type=F32)
    centre = jnp.sum(probs * g_probs, axis=-1, keepdims=True)
    g_scores = (probs * (g_probs - centre)).astype(BF16)
    g_query = jnp.einsum("gcrqk,gkcd->gqcrd", g_scores, key, preferred_element_type=F32) * scale
    g_key = jnp.einsum("gcrqk,gqcrd->gkcd", g_scores, query, preferred_element_type=F32) * scale
    g_value = jnp.einsum(
        "gcrqk,gqcrd->gkcd", probs.astype(BF16), g_heads, preferred_element_type=F32
    )
    g_qkv = jnp.concatenate(
        [
            rotate(g_query.reshape(groups, full_len, heads, HD), cos_h, -sin_h).reshape(tokens, -1),
            rotate(g_key, cos_h, -sin_h).reshape(tokens, -1),
            g_value.reshape(tokens, -1),
        ],
        axis=1,
    ).astype(BF16)
    qkv_exit_grad = token_sum(en_qkv, g_qkv)
    total = scatter_tokens(jnp.concatenate([dot_t(g_qkv, w_qkv), dot_t(g_qkv, e_qkv)], axis=1))
    g_en_qkv = (select_own * total[:, width:]).astype(BF16)
    g_one = total[:, :width] + dot_t(g_en_qkv, qkv_in)
    input_grad = from_layer((g_mid + norm_back(inputs, gain_one, g_one)).astype(BF16))
    qkv_entry_grad = token_sum(rows_of(n1), gather_tokens(g_en_qkv))

    exits = jnp.concatenate(
        [qkv_exit_grad, attn_entry_grad, gate_exit_grad, up_exit_grad, down_entry_grad], axis=1
    )
    cols = exits.shape[1]
    per = ranks // (n_s * n_c)
    exits = lax.psum_scatter(
        exits.reshape(n_s, n_c, per, cols).transpose(1, 0, 2, 3), "context", scatter_dimension=0
    )
    exits = lax.all_to_all(exits, "shard", 0, 0, tiled=True)

    def join(first, count):
        part = exits[:, :, first : first + count]
        return part.transpose(1, 0, 2).reshape(per, n_s * count)

    def join_kv(first):
        part = exits[:, :, first : first + k_cols]
        copies = n_s * kv_take // kv_heads_here
        part = part.reshape(n_s // copies, copies, per, k_cols).sum(axis=1)
        return part.transpose(1, 0, 2).reshape(per, kv_heads_here * HD)

    a = q_cols + 2 * k_cols
    f = a + q_cols
    rows = lax.psum_scatter(
        jnp.concatenate(
            [qkv_entry_grad, attn_exit_grad, gate_entry_grad, up_entry_grad, down_exit_grad], axis=1
        ).reshape(n_c, block, 5 * ranks),
        "context",
        scatter_dimension=0,
    )
    qkv_eg, attn_xg, gate_eg, up_eg, down_xg = (
        rows[:, i * ranks : (i + 1) * ranks] for i in range(5)
    )
    return (
        layer_out,
        input_grad,
        qkv_eg,
        join(0, q_cols),
        join_kv(q_cols),
        join_kv(q_cols + k_cols),
        join(a, q_cols),
        attn_xg,
        gate_eg,
        join(f, f_cols),
        up_eg,
        join(f + f_cols, f_cols),
        join(f + 2 * f_cols, f_cols),
        down_xg,
    )


def solution(mesh):
    in_specs = (
        P("shard", "context", None),
        P("shard", "context", None),
        P("shard"),
        P("shard"),
        P(),
        P(),
        P(("shard", "context"), "tensor"),
        P(("shard", "context"), "tensor"),
        P(("shard", "context"), "tensor"),
        P(("shard", "context"), "tensor"),
        P(("shard", "context"), "tensor"),
        P(("shard", "context"), "tensor"),
        P(("shard", "context"), "tensor"),
        P(("shard", "context"), None),
        P(("shard", "context"), "tensor"),
        P(("shard", "context"), "tensor"),
        P(("shard", "context"), "tensor"),
        P(("shard", "context"), "tensor"),
        P(("shard", "context"), None),
        P(("shard", "context"), None),
        P(("shard", "context"), "tensor"),
        P(("shard", "context"), None),
        P(("shard", "context"), "tensor"),
        P(("shard", "context"), "tensor"),
        P(("shard", "context"), None),
    )
    out_specs = (
        P("shard", "context", None),
        P("shard", "context", None),
        P(("shard", "context"), None),
        P(("shard", "context"), "tensor"),
        P(("shard", "context"), "tensor"),
        P(("shard", "context"), "tensor"),
        P(("shard", "context"), "tensor"),
        P(("shard", "context"), None),
        P(("shard", "context"), None),
        P(("shard", "context"), "tensor"),
        P(("shard", "context"), None),
        P(("shard", "context"), "tensor"),
        P(("shard", "context"), "tensor"),
        P(("shard", "context"), None),
    )
    return jax.shard_map(shards, mesh=mesh, in_specs=in_specs, out_specs=out_specs, check_vma=False)
```

```python
import functools
import math

import jax
import jax.numpy as jnp
from jax import lax
from jax.experimental import pallas as pl
from jax.experimental.pallas import tpu as pltpu
from jax.sharding import PartitionSpec as P

HD = 128
RANK = 16
EPSILON = 1e-05
ROPE_BASE = 1000000.0
MASKED = -1e30
F32 = jnp.float32
BF16 = jnp.bfloat16
MESH = pl.DeviceIdType.MESH


def dot(left, right):
    return jnp.dot(left, right, preferred_element_type=F32)


def dot_t(left, right):
    return lax.dot_general(left, right, (((1,), (1,)), ((), ())), preferred_element_type=F32)


def token_sum(left, right):
    return lax.dot_general(left, right, (((0,), (0,)), ((), ())), preferred_element_type=F32)


def rms_scale(values, gain):
    return values * lax.rsqrt(jnp.mean(values * values, axis=-1, keepdims=True) + EPSILON) * gain


def norm_back(values, gain, grad):
    r = lax.rsqrt(jnp.mean(values * values, axis=-1, keepdims=True) + EPSILON)
    scaled = grad * gain
    return r * scaled - values * (r * r * r * jnp.mean(values * scaled, axis=-1, keepdims=True))


def rope(values, cosine, sine):
    return values * cosine + pltpu.roll(values, HD // 2, 1) * sine


def head_tables(positions):
    half = HD // 2
    inverse = ROPE_BASE ** (-2.0 * jnp.arange(half).astype(F32) / HD)
    angles = positions.astype(F32)[:, None] * inverse[None, :]
    cosine, sine = jnp.cos(angles), jnp.sin(angles)
    return jnp.concatenate([cosine, cosine], axis=1), jnp.concatenate([-sine, sine], axis=1)


def masked_scores(query, key, length, first):
    rows, keys = query.shape[0], key.shape[0]
    scores = dot_t(query, key) * (1.0 / math.sqrt(HD))
    at = first + lax.broadcasted_iota(jnp.int32, (rows, keys), 0)
    to = lax.broadcasted_iota(jnp.int32, (rows, keys), 1)
    return jnp.where((to <= at) & (to < length), scores, MASKED)


def attend_kernel(heads, kv_heads, tile, lengths, qkv_ref, cos_ref, sin_ref, att_ref, low_ref, lse_ref):
    length = lengths[pl.program_id(0)]
    full_len = qkv_ref.shape[0]
    for h in range(heads + kv_heads):
        cols = slice(h * HD, (h + 1) * HD)
        low_ref[:, cols] = rope(qkv_ref[:, cols], cos_ref[...], sin_ref[...]).astype(BF16)
    first_value = (heads + kv_heads) * HD
    low_ref[:, first_value:] = qkv_ref[:, first_value:].astype(BF16)
    lse_ref[...] = jnp.zeros_like(lse_ref)
    for first in range(0, full_len, tile):
        rows, keys = slice(first, first + tile), slice(0, first + tile)
        for h in range(heads):
            kv = h * kv_heads // heads
            key = low_ref[keys, (heads + kv) * HD : (heads + kv + 1) * HD]
            value = low_ref[keys, first_value + kv * HD : first_value + (kv + 1) * HD]
            scores = masked_scores(low_ref[rows, h * HD : (h + 1) * HD], key, length, first)
            largest = jnp.max(scores, axis=1, keepdims=True)
            exponent = jnp.exp(scores - largest)
            total = jnp.sum(exponent, axis=1, keepdims=True)
            probs = (exponent / total).astype(BF16)
            att_ref[rows, h * HD : (h + 1) * HD] = dot(probs, value).astype(BF16)
            lse_ref[rows, h : h + 1] = largest + jnp.log(total)


def attend_back_kernel(
    heads, kv_heads, tile, lengths, low_ref, lse_ref, g_ref, cos_ref, sin_ref, out_ref, k_acc, v_acc
):
    length = lengths[pl.program_id(0)]
    full_len = low_ref.shape[0]
    first_value = (heads + kv_heads) * HD
    scale = 1.0 / math.sqrt(HD)
    k_acc[...] = jnp.zeros_like(k_acc)
    v_acc[...] = jnp.zeros_like(v_acc)
    for first in range(0, full_len, tile):
        rows, keys = slice(first, first + tile), slice(0, first + tile)
        for h in range(heads):
            kv = h * kv_heads // heads
            kv_cols = slice(kv * HD, (kv + 1) * HD)
            key = low_ref[keys, (heads + kv) * HD : (heads + kv + 1) * HD]
            value = low_ref[keys, first_value + kv * HD : first_value + (kv + 1) * HD]
            query = low_ref[rows, h * HD : (h + 1) * HD]
            grad = g_ref[rows, h * HD : (h + 1) * HD]
            probs = jnp.exp(masked_scores(query, key, length, first) - lse_ref[rows, h : h + 1])
            g_probs = dot_t(grad, value)
            centre = jnp.sum(probs * g_probs, axis=1, keepdims=True)
            g_scores = (probs * (g_probs - centre)).astype(BF16)
            g_query = dot(g_scores, key) * scale
            out_ref[rows, h * HD : (h + 1) * HD] = rope(
                g_query, cos_ref[rows, :], -sin_ref[rows, :]
            ).astype(BF16)
            k_acc[keys, kv_cols] += token_sum(g_scores, query)
            v_acc[keys, kv_cols] += token_sum(probs.astype(BF16), grad)
    for kv in range(kv_heads):
        cols = slice(kv * HD, (kv + 1) * HD)
        out_ref[:, (heads + kv) * HD : (heads + kv + 1) * HD] = rope(
            k_acc[:, cols] * scale, cos_ref[...], -sin_ref[...]
        ).astype(BF16)
    out_ref[:, first_value:] = v_acc[...].astype(BF16)


def attention(qkv, lengths, groups, heads, kv_heads, tables):
    tokens, cols = qkv.shape
    full_len = tokens // groups
    tile = min(256, full_len)

    def seq(width):
        return pl.BlockSpec((full_len, width), lambda g, lens: (g, 0))

    table = pl.BlockSpec((full_len, HD), lambda g, lens: (0, 0))
    params = pltpu.CompilerParams(vmem_limit_bytes=56 * 1024 * 1024)
    att, low, lse = pl.pallas_call(
        functools.partial(attend_kernel, heads, kv_heads, tile),
        out_shape=(
            jax.ShapeDtypeStruct((tokens, heads * HD), BF16),
            jax.ShapeDtypeStruct((tokens, cols), BF16),
            jax.ShapeDtypeStruct((tokens, HD), F32),
        ),
        grid_spec=pltpu.PrefetchScalarGridSpec(
            num_scalar_prefetch=1,
            grid=(groups,),
            in_specs=[seq(cols), table, table],
            out_specs=[seq(heads * HD), seq(cols), seq(HD)],
        ),
        compiler_params=params,
        name="attend",
    )(lengths, qkv, *tables)

    def backward(grad):
        return pl.pallas_call(
            functools.partial(attend_back_kernel, heads, kv_heads, tile),
            out_shape=jax.ShapeDtypeStruct((tokens, cols), BF16),
            grid_spec=pltpu.PrefetchScalarGridSpec(
                num_scalar_prefetch=1,
                grid=(groups,),
                in_specs=[seq(cols), seq(HD), seq(heads * HD), table, table],
                out_specs=seq(cols),
                scratch_shapes=[
                    pltpu.VMEM((full_len, kv_heads * HD), F32),
                    pltpu.VMEM((full_len, kv_heads * HD), F32),
                ],
            ),
            compiler_params=params,
            name="attend_back",
        )(lengths, low, lse, grad, *tables)

    return att, backward


def ring_at(i, n):
    upper = i // (n // 2)
    return (1 - upper) * 2 * i + upper * (2 * (n - 1 - i) + 1)


def ring_pos(s, n):
    return (1 - s % 2) * (s // 2) + (s % 2) * (n - 1 - s // 2)


def greet(targets):
    barrier = pltpu.get_barrier_semaphore()
    for target in targets:
        pl.semaphore_signal(barrier, inc=1, device_id=target, device_id_type=MESH)
    pl.semaphore_wait(barrier, len(targets))


def send_to(source, target, send_sem, recv_sem, device):
    return pltpu.make_async_remote_copy(
        source, target, send_sem, recv_sem, device_id=device, device_id_type=MESH
    )


def xor(a, b, n):
    total, bit = 0, 1
    while bit < n:
        total = total + ((a // bit + b // bit) % 2) * bit
        bit *= 2
    return total


def home(q, z, k, n):
    return xor(xor(q, z, n), k * (n // 2), n)


def halves(ref, k):
    length = ref.shape[-2] // 2
    return pl.ds(k * length, length)


def others(n, n_c):
    me = lax.axis_index("shard") * n_c + lax.axis_index("context")
    peers = []
    for k in range(1, n * n_c):
        i = (me + k) % (n * n_c)
        peers.append({"shard": i // n_c, "context": i % n_c})
    return peers


class Exchange:
    def __init__(self, n, n_c, source, target, send_sem, recv_sem, own_sem, same):
        s, c = lax.axis_index("shard"), lax.axis_index("context")
        everyone = n * n_c
        me = s * n_c + c
        self.copies, self.arrivals = [], []
        for k, peer in enumerate(others(n, n_c), 1):
            to = (peer["shard"],) if same else (peer["shard"], peer["context"])
            self.copies.append(
                send_to(source.at[to], target.at[s, c], send_sem.at[k], recv_sem.at[k], peer)
            )
            i = (me + everyone - k) % everyone
            slot = target.at[i // n_c, i % n_c]
            self.arrivals.append(send_to(slot, slot, send_sem.at[k], recv_sem.at[k], peer))
        mine = source.at[s] if same else source.at[s, c]
        self.own = pltpu.make_async_copy(mine, target.at[s, c], own_sem.at[0])

    def start(self):
        for copy in self.copies:
            copy.start()
        self.own.start()

    def finish(self):
        self.own.wait()
        for copy in self.arrivals:
            copy.wait_recv()
        for copy in self.copies:
            copy.wait_send()

    @staticmethod
    def sems(n, n_c):
        dma = pltpu.SemaphoreType.DMA
        return [dma((n * n_c,)), dma((n * n_c,)), dma((1,))]


class Arrive:
    def __init__(self, n, source, middle, target, sems):
        self.s, self.c = lax.axis_index("shard"), lax.axis_index("context")
        self.to = [home(self.s, self.c, k, n) for k in (0, 1)]
        self.first, self.second, self.local = [], [], []
        for k in (0, 1):
            rows = halves(source, k)
            self.first.append(
                send_to(
                    source.at[rows], middle.at[rows], sems.at[0, k], sems.at[1, k],
                    {"shard": self.to[k]},
                )
            )
            self.second.append(
                send_to(
                    middle.at[rows], target.at[rows], sems.at[2, k], sems.at[3, k],
                    {"context": self.to[k]},
                )
            )
            self.local.append(
                (
                    pltpu.make_async_copy(source.at[rows], middle.at[rows], sems.at[4, k]),
                    pltpu.make_async_copy(middle.at[rows], target.at[rows], sems.at[5, k]),
                )
            )

    def either(self, stage, k, remote, local):
        own = self.s if stage == 0 else self.c
        pl.when(self.to[k] != own)(remote)
        pl.when(self.to[k] == own)(local)

    def start(self):
        for k in (0, 1):
            self.either(0, k, self.first[k].start, self.local[k][0].start)

    def relay(self):
        for k in (0, 1):
            self.either(0, k, self.first[k].wait_recv, self.local[k][0].wait)
            self.either(1, k, self.second[k].start, self.local[k][1].start)

    def finish(self):
        for k in (0, 1):
            self.either(0, k, self.first[k].wait_send, lambda: None)

            def both(copy=self.second[k]):
                copy.wait_send()
                copy.wait_recv()

            self.either(1, k, both, self.local[k][1].wait)

    @staticmethod
    def scratch(shape):
        return [pltpu.VMEM(shape, BF16), pltpu.SemaphoreType.DMA((6, 2))]


class Depart:
    def __init__(self, n, source, target, sems):
        s, c, t = (lax.axis_index(name) for name in ("shard", "context", "tensor"))
        self.stays, self.away, self.kept, self.passed, self.got = [], [], [], [], []
        for k in (0, 1):
            rows = halves(source, k)
            block = home(s, c, k, n)
            self.stays.append((s == c) & (block == s))
            self.away.append(
                send_to(
                    source.at[rows], target.at[t, rows], sems.at[0, k], sems.at[1, k],
                    {"shard": c, "context": block},
                )
            )
            self.kept.append(
                pltpu.make_async_copy(source.at[rows], target.at[t, rows], sems.at[4, k])
            )
            for core, group in ((t, self.passed), (1 - t, self.got)):
                spot = target.at[core, rows]
                group.append(
                    send_to(spot, spot, sems.at[2, k], sems.at[3, k], {"tensor": 1 - t})
                )

    def start(self):
        for k in (0, 1):
            pl.when(~self.stays[k])(self.away[k].start)
            pl.when(self.stays[k])(self.kept[k].start)

    def finish(self):
        for k in (0, 1):
            pl.when(~self.stays[k])(self.away[k].wait_recv)
            pl.when(self.stays[k])(self.kept[k].wait)
            self.passed[k].start()
        for k in (0, 1):
            self.got[k].wait_recv()
            self.passed[k].wait_send()
            pl.when(~self.stays[k])(self.away[k].wait_send)

    @staticmethod
    def sems():
        return [pltpu.SemaphoreType.DMA((5, 2))]


def neighbours(n):
    pos = ring_pos(lax.axis_index("shard"), n)
    sides = tuple({"shard": ring_at((pos + step) % n, n)} for step in (1, n - 1))
    return pos, sides, {"tensor": 1 - lax.axis_index("tensor")}


def ring_steps(n):
    half = n // 2
    steps = []
    for d in range(1, half + 1):
        steps += [(0, d, 0), (1, d, 1)]
        if d < half:
            steps += [(0, d, 1), (1, d, 0)]
    return steps


def gather_kernel(n, count, *refs):
    sources, outs = refs[:count], refs[count : 2 * count]
    ring_send, ring_recv, pair_send, pair_recv, own_sem = refs[2 * count :]
    half_len = sources[0].shape[0] // 2
    steps = ring_steps(n)
    t = lax.axis_index("tensor")
    pos, sides, partner = neighbours(n)
    greet(sides + (partner,))
    arrays = range(count)

    def rows(k):
        return pl.ds(k * half_len, half_len)

    layer = lax.axis_index("context")

    def place(a, core, who, k):
        return outs[a].at[core, home(ring_at(who % n, n), layer, k, n), rows(k)]

    def origin(way, d):
        return pos + (n - d if way == 0 else d)

    def sent(a, way, d, k):
        spot = place(a, t, origin(way, d - 1), k)
        source = sources[a].at[rows(k)] if d == 1 else spot
        at = (a, way, d - 1, k)
        return send_to(source, spot, ring_send.at[at], ring_recv.at[at], sides[way])

    def got(a, way, d, k):
        spot, at = place(a, t, origin(way, d), k), (a, way, d - 1, k)
        return send_to(spot, spot, ring_send.at[at], ring_recv.at[at], sides[way])

    def pair(a, core, way, d, k, source=None):
        spot, at = place(a, core, origin(way, d), k), (a, way, d, k)
        return send_to(
            spot if source is None else source, spot, pair_send.at[at], pair_recv.at[at], partner
        )

    waits = []
    for step in steps:
        if step[1] == 1:
            for a in arrays:
                waits.append(sent(a, *step))
                waits[-1].start()
    own = []
    for a in arrays:
        for k in (0, 1):
            waits.append(pair(a, t, 0, 0, k, sources[a].at[rows(k)]))
            waits[-1].start()
            own.append(
                pltpu.make_async_copy(sources[a].at[rows(k)], place(a, t, pos, k), own_sem.at[a, k])
            )
            own[-1].start()
    for way, d, k in steps:
        for a in arrays:
            got(a, way, d, k).wait_recv()
            if (way, d + 1, k) in steps:
                waits.append(sent(a, way, d + 1, k))
                waits[-1].start()
            waits.append(pair(a, t, way, d, k))
            waits[-1].start()
    for a in arrays:
        for step in [(0, 0, 0), (0, 0, 1)] + steps:
            pair(a, 1 - t, *step).wait_recv()
    for copy in waits:
        copy.wait_send()
    for copy in own:
        copy.wait()


def gather_tokens(call, *values):
    n, count, half = lax.axis_size("shard"), len(values), lax.axis_size("shard") // 2
    dma = pltpu.SemaphoreType.DMA
    outs = pl.pallas_call(
        functools.partial(gather_kernel, n, count),
        out_shape=[jax.ShapeDtypeStruct((2, n) + v.shape, v.dtype) for v in values],
        in_specs=[pl.BlockSpec(memory_space=pltpu.VMEM)] * count,
        out_specs=[pl.BlockSpec(memory_space=pl.ANY)] * count,
        scratch_shapes=[
            dma((count, 2, half, 2)),
            dma((count, 2, half, 2)),
            dma((count, 2, half + 1, 2)),
            dma((count, 2, half + 1, 2)),
            dma((count, 2)),
        ],
        compiler_params=pltpu.CompilerParams(collective_id=call, has_side_effects=True),
        cost_estimate=pl.CostEstimate(flops=0, bytes_accessed=100_000_000, transcendentals=0),
        name=f"gather_{call}",
    )(*values)
    return [out.reshape(2 * n * v.shape[0], v.shape[1]) for out, v in zip(outs, values)]


def scatter_tokens(call, *values, depart=None, exits=None):
    n, n_c, count = lax.axis_size("shard"), lax.axis_size("context"), len(values)
    cols = sum(v.shape[1] for v in values)
    length = values[0].shape[0] // (2 * n)
    half, half_len = n // 2, length // 2
    steps = ring_steps(n)

    def kernel(*refs):
        refs = list(refs)
        parts = [refs.pop(0) for _ in range(count)]
        depart_ref = refs.pop(0) if depart is not None else None
        exits_ref = refs.pop(0) if exits is not None else None
        out_ref = refs.pop(0)
        depart_out = refs.pop(0) if depart is not None else None
        exits_out = refs.pop(0) if exits is not None else None
        mine, other, outbox, inbox = [refs.pop(0) for _ in range(4)]
        ring_send, ring_recv, pair_send, pair_recv, load_sem = [refs.pop(0) for _ in range(5)]
        t = lax.axis_index("tensor")
        layer = lax.axis_index("context")
        pos, sides, partner = neighbours(n)
        jobs = []
        if depart is not None:
            jobs.append(Depart(n, depart_ref, depart_out, refs.pop(0)))
        if exits is not None:
            exits_in = refs.pop(0)
            jobs.append(
                Exchange(n, n_c, exits_ref, exits_in, *(refs.pop(0) for _ in range(3)), False)
            )
        greet((others(n, n_c) if jobs else list(sides)) + [partner])
        order = [half]
        for d in range(half - 1, 0, -1):
            order += [d, n - d]
        order.append(0)

        def rows(k):
            return pl.ds(k * half_len, half_len)

        swaps, loads = {}, {}
        for d in order:
            who = ring_at((pos + d) % n, n)
            swaps[d], loads[d], first = [], [], 0
            for a, part in enumerate(parts):
                cols_a = pl.ds(first, part.shape[-1])
                first += part.shape[-1]
                for k in (0, 1):
                    at = (a, d, k)
                    block = home(who, layer, k, n)
                    loads[d].append(
                        pltpu.make_async_copy(
                            part.at[t, block, rows(k)], mine.at[d, rows(k), cols_a], load_sem.at[at]
                        )
                    )
                    swaps[d].append(
                        send_to(
                            part.at[1 - t, block, rows(k)], other.at[d, rows(k), cols_a],
                            pair_send.at[at], pair_recv.at[at], partner,
                        )
                    )
                    swaps[d][-1].start()
                    loads[d][-1].start()
        for job in jobs:
            job.start()

        def ready(d):
            for copy in loads[d]:
                copy.wait()
            for copy in swaps[d]:
                copy.wait_recv()

        def chip_sum(d, k):
            return mine[d, rows(k), :].astype(F32) + other[d, rows(k), :].astype(F32)

        def ring(way, d, k):
            at = (way, d - 1, k)
            box = (way, d - 1, rows(k))
            return send_to(
                outbox.at[box], inbox.at[box], ring_send.at[at], ring_recv.at[at], sides[way]
            )

        def send(way, d, k, total):
            outbox[way, d - 1, rows(k), :] = total.astype(BF16)
            ring(way, d, k).start()

        def taken(way, d, k):
            ring(way, d, k).wait_recv()
            return inbox[way, d - 1, rows(k), :].astype(F32)

        ready(half)
        send(0, half, 0, chip_sum(half, 0))
        send(1, half, 1, chip_sum(half, 1))
        for d in range(half - 1, 0, -1):
            for way, index in ((0, d), (1, n - d)):
                ready(index)
                k = 1 - way
                total = chip_sum(index, k)
                if (way, d + 1, k) in steps:
                    total = total + taken(way, d + 1, k)
                send(way, d, k, total)
            for way, index in ((0, d), (1, n - d)):
                send(way, d, way, chip_sum(index, way) + taken(way, d + 1, way))
        ready(0)
        for k in (0, 1):
            out_ref[rows(k), :] = chip_sum(0, k)
        for way, k in ((0, 1), (1, 0), (0, 0), (1, 1)):
            out_ref[rows(k), :] += taken(way, 1, k)
        for step in steps:
            ring(*step).wait_send()
        for d in order:
            for copy in swaps[d]:
                copy.wait_send()
        for job in jobs:
            job.finish()
        if exits is not None:
            add_layers(exits_in, exits_out)

    dma = pltpu.SemaphoreType.DMA
    any_space, vmem = pl.BlockSpec(memory_space=pl.ANY), pl.BlockSpec(memory_space=pltpu.VMEM)
    operands = [v.astype(BF16).reshape(2, n, length, v.shape[1]) for v in values]
    in_specs, out_specs = [any_space] * count, [vmem]
    out_shape = [jax.ShapeDtypeStruct((length, cols), F32)]
    scratch = [
        pltpu.VMEM((n, length, cols), BF16),
        pltpu.VMEM((n, length, cols), BF16),
        pltpu.VMEM((2, half, length, cols), BF16),
        pltpu.VMEM((2, half, length, cols), BF16),
        dma((2, half, 2)),
        dma((2, half, 2)),
        dma((count, n, 2)),
        dma((count, n, 2)),
        dma((count, n, 2)),
    ]
    if depart is not None:
        operands.append(depart)
        in_specs.append(vmem)
        out_specs.append(any_space)
        out_shape.append(jax.ShapeDtypeStruct((2,) + depart.shape, BF16))
        scratch += Depart.sems()
    if exits is not None:
        operands.append(exits)
        in_specs.append(vmem)
        out_specs.append(vmem)
        out_shape.append(jax.ShapeDtypeStruct((n,) + exits.shape[2:], F32))
        scratch += [pltpu.VMEM(exits.shape, BF16)] + Exchange.sems(n, n_c)
    return pl.pallas_call(
        kernel,
        out_shape=out_shape,
        in_specs=in_specs,
        out_specs=out_specs,
        scratch_shapes=scratch,
        compiler_params=pltpu.CompilerParams(
            collective_id=call, has_side_effects=True, vmem_limit_bytes=52 * 1024 * 1024
        ),
        cost_estimate=pl.CostEstimate(flops=0, bytes_accessed=100_000_000, transcendentals=0),
        name=f"scatter_{call}",
    )(*operands)


def add_layers(inbox, out_ref):
    for q in range(inbox.shape[0]):
        total = inbox[q, 0].astype(F32)
        for i in range(1, inbox.shape[1]):
            total = total + inbox[q, i].astype(F32)
        out_ref[q] = total


def spread(call, sources, items, widths, tokens, wide=None):
    n, n_c = lax.axis_size("shard"), lax.axis_size("context")
    n_in, n_out = len(sources), len(widths)
    rows = sources[0].shape[0]

    def kernel(*refs):
        refs = list(refs)
        ins = [refs.pop(0) for _ in range(n_in)]
        tokens_ref = refs.pop(0)
        wide_ref = refs.pop(0) if wide is not None else None
        outs = [refs.pop(0) for _ in range(n_out)]
        tokens_out = refs.pop(0)
        wide_out = refs.pop(0) if wide is not None else None
        send_sem, recv_sem, own_sem = refs.pop(0), refs.pop(0), refs.pop(0)
        arrive = Arrive(n, tokens_ref, refs.pop(0), tokens_out, refs.pop(0))
        s = lax.axis_index("shard")
        exchange = None
        if wide is not None:
            exchange = Exchange(
                n, n_c, wide_ref, wide_out, *(refs.pop(0) for _ in range(3)), True
            )
        bounce = refs
        greet(others(n, n_c))

        def piece(item, q):
            source, _, _, width, kind, heads = items[item]
            if kind == "split":
                first = pl.multiple_of(q * width, HD)
            elif kind == "kv":
                first = pl.multiple_of((q * heads // n) * HD, HD)
            else:
                first = 0
            return ins[source].at[:, pl.ds(first, width)]

        def spot(item, q):
            _, out, first, width, _, _ = items[item]
            return outs[out].at[q, :, pl.ds(first, width)]

        arrive.start()
        waits, own, arrivals = [], [], []
        for item in range(len(items)):
            for k in range(1, n):
                q = (s + k) % n
                at = (item, k)
                copy = send_to(
                    piece(item, q), spot(item, s), send_sem.at[at], recv_sem.at[at], {"shard": q}
                )
                copy.start()
                waits.append(copy)
                q = (s + n - k) % n
                arrivals.append(
                    send_to(
                        spot(item, q), spot(item, q), send_sem.at[at], recv_sem.at[at], {"shard": q}
                    )
                )
            copy = pltpu.make_async_copy(piece(item, s), bounce[item], own_sem.at[item, 0])
            copy.start()
            own.append(copy)
        if exchange is not None:
            exchange.start()
        stored = []
        for item in range(len(items)):
            own[item].wait()
            copy = pltpu.make_async_copy(bounce[item], spot(item, s), own_sem.at[item, 1])
            copy.start()
            stored.append(copy)
        arrive.relay()
        for copy in stored:
            copy.wait()
        if exchange is not None:
            exchange.finish()
        for copy in arrivals:
            copy.wait_recv()
        for copy in waits:
            copy.wait_send()
        arrive.finish()

    dma = pltpu.SemaphoreType.DMA
    any_space, vmem = pl.BlockSpec(memory_space=pl.ANY), pl.BlockSpec(memory_space=pltpu.VMEM)
    scratch = [dma((len(items), n)), dma((len(items), n)), dma((len(items), 2))]
    scratch += Arrive.scratch(tokens.shape)
    out_shape = [jax.ShapeDtypeStruct((n, rows, w), BF16) for w in widths]
    out_shape.append(jax.ShapeDtypeStruct(tokens.shape, BF16))
    operands = list(sources) + [tokens]
    if wide is not None:
        operands.append(wide)
        scratch += Exchange.sems(n, n_c)
        out_shape.append(jax.ShapeDtypeStruct((n, n_c) + wide.shape[1:], BF16))
    scratch += [pltpu.VMEM((rows, item[3]), BF16) for item in items]
    return pl.pallas_call(
        kernel,
        out_shape=out_shape,
        in_specs=[any_space] * n_in + [vmem] * (len(operands) - n_in),
        out_specs=[any_space] * len(out_shape),
        scratch_shapes=scratch,
        compiler_params=pltpu.CompilerParams(collective_id=call, has_side_effects=True),
        cost_estimate=pl.CostEstimate(flops=0, bytes_accessed=40_000_000, transcendentals=0),
        name=f"spread_{call}",
    )(*operands)


def collect(call, exits, rows, depart):
    n, n_c = exits.shape[:2]

    def kernel(
        exits_ref, rows_ref, depart_ref, exits_out, rows_out, depart_out, exits_in, rows_in, *sems
    ):
        c = lax.axis_index("context")
        leave = Depart(n, depart_ref, depart_out, sems[0])
        exchange = Exchange(n, n_c, exits_ref, exits_in, *sems[1:4], False)
        greet(others(n, n_c) + [{"tensor": 1 - lax.axis_index("tensor")}])
        leave.start()
        waits, arrivals = [], []
        for k in range(1, n_c):
            to, via = (c + k) % n_c, (c + n_c - k) % n_c
            at = (sems[4].at[0, k], sems[4].at[1, k])
            waits.append(send_to(rows_ref.at[to], rows_in.at[c], *at, {"context": to}))
            waits[-1].start()
            arrivals.append(send_to(rows_in.at[via], rows_in.at[via], *at, {"context": to}))
        exchange.start()
        kept = pltpu.make_async_copy(rows_ref.at[c], rows_in.at[c], sems[4].at[0, 0])
        kept.start()
        kept.wait()
        for copy in arrivals:
            copy.wait_recv()
        total = rows_in[0].astype(F32)
        for i in range(1, n_c):
            total = total + rows_in[i].astype(F32)
        rows_out[...] = total
        exchange.finish()
        add_layers(exits_in, exits_out)
        leave.finish()
        for copy in waits:
            copy.wait_send()

    vmem = pl.BlockSpec(memory_space=pltpu.VMEM)
    return pl.pallas_call(
        kernel,
        out_shape=(
            jax.ShapeDtypeStruct((n,) + exits.shape[2:], F32),
            jax.ShapeDtypeStruct(rows.shape[1:], F32),
            jax.ShapeDtypeStruct((2,) + depart.shape, BF16),
        ),
        in_specs=[vmem] * 3,
        out_specs=(vmem, vmem, pl.BlockSpec(memory_space=pl.ANY)),
        scratch_shapes=[pltpu.VMEM(exits.shape, BF16), pltpu.VMEM(rows.shape, BF16)]
        + Depart.sems()
        + Exchange.sems(n, n_c)
        + [pltpu.SemaphoreType.DMA((2, n_c))],
        compiler_params=pltpu.CompilerParams(collective_id=call, has_side_effects=True),
        cost_estimate=pl.CostEstimate(flops=0, bytes_accessed=60_000_000, transcendentals=0),
        name=f"collect_{call}",
    )(exits, rows, depart)


def entry_grads(pairs, n_s, n_c, s):
    tokens, width = pairs[0][0].shape
    block = width // (n_s * n_c)
    if block % HD:
        parts = []
        for acts, side in pairs:
            mine = lax.dynamic_index_in_dim(
                acts.reshape(tokens, n_c, n_s, block), s, 2, keepdims=False
            )
            parts.append(token_sum(mine.reshape(tokens, n_c * block), side))
        return jnp.concatenate(parts, axis=1).astype(BF16).reshape(n_c, block, -1)
    count = len(pairs)
    total = sum(side.shape[1] for _, side in pairs)

    def kernel(_, *refs):
        first = 0
        for a in range(count):
            cols = slice(first, first + refs[count + a].shape[1])
            first = cols.stop
            refs[-1][0, :, cols] = token_sum(refs[a][...], refs[count + a][...]).astype(BF16)

    return pl.pallas_call(
        kernel,
        out_shape=jax.ShapeDtypeStruct((n_c, block, total), BF16),
        grid_spec=pltpu.PrefetchScalarGridSpec(
            num_scalar_prefetch=1,
            grid=(n_c,),
            in_specs=[pl.BlockSpec((tokens, block), lambda i, at: (0, i * n_s + at[0]))] * count
            + [pl.BlockSpec(side.shape, lambda i, at: (0, 0)) for _, side in pairs],
            out_specs=pl.BlockSpec((1, block, total), lambda i, at: (i, 0, 0)),
        ),
        name="entry_grads",
    )(s.reshape(1).astype(jnp.int32), *(a for a, _ in pairs), *(b for _, b in pairs))


def shards(
    hidden_in,
    cotangent,
    seq_lengths,
    adapter_ids,
    attn_gain,
    ffn_gain,
    query_weight,
    key_weight,
    value_weight,
    output_weight,
    gate_weight,
    up_weight,
    down_weight,
    qkv_entry,
    query_exit,
    key_exit,
    value_exit,
    attn_entry,
    attn_exit,
    gate_entry,
    gate_exit,
    up_entry,
    up_exit,
    down_entry,
    down_exit,
):
    n_s, n_c = lax.axis_size("shard"), lax.axis_size("context")
    s, t = lax.axis_index("shard"), lax.axis_index("tensor")
    groups, local_len, width = hidden_in.shape
    block = width // (n_s * n_c)
    full_len = local_len * n_c
    tokens = groups * full_len
    ranks = qkv_entry.shape[1]
    swap = [(a * n_c + b, b * n_c + a) for a in range(n_s) for b in range(n_c)]

    def own_tokens(values):
        own = lax.dynamic_index_in_dim(values, t, 0, keepdims=False)
        own = own.reshape(local_len, n_s, n_c, block).transpose(0, 2, 1, 3)
        return own.reshape(local_len, width)

    def as_output(values):
        swapped = values.reshape(2, local_len, n_c, n_s, block).transpose(0, 1, 3, 2, 4)
        return swapped.reshape(2, local_len, width)

    def features(vector):
        return vector.reshape(n_s, n_c, block).transpose(1, 0, 2).reshape(width).astype(F32)

    q_cols = query_weight.shape[1] // n_s
    f_cols = gate_weight.shape[1] // n_s
    kv_here = key_weight.shape[1] // HD
    kv_take = max(1, kv_here // n_s)
    k_cols = kv_take * HD
    heads = q_cols // HD
    a_cols = q_cols + 2 * k_cols

    def split(weights):
        rows, cols = weights.shape
        return weights.reshape(rows, n_s, cols // n_s).transpose(1, 0, 2)

    def split_kv(weights):
        first = [q * kv_here // n_s * HD for q in range(n_s)]
        return jnp.stack([weights[:, at : at + k_cols] for at in first])

    exit_pack = jnp.concatenate(
        [
            split(query_exit),
            split_kv(key_exit),
            split_kv(value_exit),
            split(attn_entry),
            split(gate_exit),
            split(up_exit),
            split(down_entry),
        ],
        axis=2,
    )
    entry_a = jnp.where(t == 0, qkv_entry, attn_exit)
    entry_f = jnp.where(t == 0, gate_entry, up_entry)
    attn_pack, x_low, exits = spread(
        0,
        [query_weight, key_weight, value_weight, output_weight, entry_a],
        [
            (0, 0, 0, q_cols, "split", 0),
            (1, 0, q_cols, k_cols, "kv", kv_here),
            (2, 0, q_cols + k_cols, k_cols, "kv", kv_here),
            (3, 0, a_cols, q_cols, "split", 0),
            (4, 0, a_cols + q_cols, ranks, "same", 0),
        ],
        [a_cols + q_cols + ranks],
        own_tokens(hidden_in),
        exit_pack,
    )
    gu_pack, down_pack, cot_low = spread(
        1,
        [gate_weight, up_weight, entry_f, down_exit, down_weight],
        [
            (0, 0, 0, f_cols, "split", 0),
            (1, 0, f_cols, f_cols, "split", 0),
            (2, 0, 2 * f_cols, ranks, "same", 0),
            (3, 0, 2 * f_cols + ranks, ranks, "same", 0),
            (4, 1, 0, f_cols, "split", 0),
        ],
        [2 * f_cols + 2 * ranks, f_cols],
        own_tokens(cotangent),
    )

    def along(pack):
        return lax.all_gather(pack, "context", axis=0).reshape(width, -1)

    def both_cores(mine):
        theirs = lax.ppermute(mine, "tensor", [(0, 1), (1, 0)])
        return jnp.where(t == 0, mine, theirs), jnp.where(t == 0, theirs, mine)

    attn_w = along(attn_pack)
    gu_w = along(gu_pack)
    w_d = along(down_pack)
    exits = exits.reshape(ranks, -1)
    lengths, ids = lax.ppermute(
        jnp.stack([seq_lengths, adapter_ids]), ("shard", "context"), swap
    )
    gain_one, gain_two = features(attn_gain), features(ffn_gain)
    layer, part_len = lax.axis_index("context"), local_len // 2
    positions = jnp.concatenate(
        [
            home(s, layer, k, n_s) * local_len + k * part_len + jnp.arange(part_len)
            for k in (0, 1)
        ]
    )
    valid = (positions < lengths[t]).astype(F32)[:, None]
    chosen = (jnp.arange(ranks)[None, :] // RANK == ids[:, None]).astype(F32)
    select_own = chosen[t][None, :]
    select_all = jnp.broadcast_to(chosen[:, None, :], (groups, full_len, ranks)).reshape(
        tokens, ranks
    )
    w_qkv, w_o = attn_w[:, :a_cols], attn_w[:, a_cols : a_cols + q_cols]
    e_qkv, e_o = exits[:, :a_cols], exits[:, a_cols : a_cols + q_cols]
    qkv_in, attn_out = both_cores(attn_w[:, a_cols + q_cols :])
    w_g, w_u = gu_w[:, :f_cols], gu_w[:, f_cols : 2 * f_cols]
    gate_in, up_in = both_cores(gu_w[:, 2 * f_cols : 2 * f_cols + ranks])
    down_out = gu_w[:, 2 * f_cols + ranks :]
    e_g, e_u, e_d = (
        exits[:, a_cols + q_cols + i * f_cols : a_cols + q_cols + (i + 1) * f_cols]
        for i in range(3)
    )

    inputs = x_low.astype(F32)
    (n1,) = gather_tokens(2, rms_scale(inputs, gain_one).astype(BF16))
    en_qkv = (select_all * dot(n1, qkv_in)).astype(BF16)
    qkv = dot(n1, w_qkv) + dot(en_qkv, e_qkv)
    att, attention_back = attention(
        qkv, lengths, groups, heads, kv_take, head_tables(jnp.arange(full_len))
    )
    (total,) = scatter_tokens(3, dot_t(att, w_o), dot_t(att, e_o))
    en_attn = (select_own * total[:, width:]).astype(BF16)
    mid = inputs + total[:, :width] + dot_t(en_attn, attn_out)

    n2, en_attn_all = gather_tokens(4, rms_scale(mid, gain_two).astype(BF16), en_attn)
    en_gate = (select_all * dot(n2, gate_in)).astype(BF16)
    en_up = (select_all * dot(n2, up_in)).astype(BF16)
    gate = dot(n2, w_g) + dot(en_gate, e_g)
    up = dot(n2, w_u) + dot(en_up, e_u)
    sig = jax.nn.sigmoid(gate)
    hidden = (gate * sig * up).astype(BF16)
    (total,) = scatter_tokens(5, dot_t(hidden, w_d), dot_t(hidden, e_d))
    en_down = (select_own * total[:, width:]).astype(BF16)
    layer_sum = mid + total[:, :width] + dot_t(en_down, down_out)
    out_low = (valid * layer_sum).astype(BF16)

    grad_out = valid * cot_low.astype(F32)
    (g_low,) = gather_tokens(6, grad_out.astype(BF16))
    g_en_down = (select_all * dot(g_low, down_out)).astype(BF16)
    down_entry_grad = token_sum(g_en_down, hidden)
    g_hidden = dot(g_low, w_d) + dot(g_en_down, e_d)
    g_gate = (g_hidden * up * (sig * (1.0 + gate * (1.0 - sig)))).astype(BF16)
    g_up = (g_hidden * gate * sig).astype(BF16)
    gate_exit_grad = token_sum(en_gate, g_gate)
    up_exit_grad = token_sum(en_up, g_up)
    total, layer_out = scatter_tokens(
        7,
        dot_t(g_gate, w_g) + dot_t(g_up, w_u),
        dot_t(g_gate, e_g),
        dot_t(g_up, e_u),
        depart=out_low,
    )
    g_en_gu = (
        jnp.concatenate([select_own, select_own], axis=1) * total[:, width:]
    ).astype(BF16)
    g_two = (
        total[:, :width]
        + dot_t(g_en_gu[:, :ranks], gate_in)
        + dot_t(g_en_gu[:, ranks:], up_in)
    )
    g_mid = grad_out + norm_back(mid, gain_two, g_two)
    g_mid_all, side = gather_tokens(
        8, g_mid.astype(BF16), jnp.concatenate([g_en_gu, en_down], axis=1)
    )
    rows_mid = entry_grads(
        [(n2, side[:, : 2 * ranks]), (g_low, side[:, 2 * ranks :]), (g_mid_all, en_attn_all)],
        n_s,
        n_c,
        s,
    )

    g_en_attn = (select_all * dot(g_mid_all, attn_out)).astype(BF16)
    attn_entry_grad = token_sum(g_en_attn, att)
    g_att = (dot(g_mid_all, w_o) + dot(g_en_attn, e_o)).astype(BF16)
    g_qkv = attention_back(g_att)
    qkv_exit_grad = token_sum(en_qkv, g_qkv)
    per = ranks // (n_s * n_c)

    def by_owner(*grads):
        packed = jnp.concatenate([grad.astype(BF16) for grad in grads], axis=1)
        return packed.reshape(n_s, n_c, per, -1)

    total, ffn_grads = scatter_tokens(
        9,
        dot_t(g_qkv, w_qkv),
        dot_t(g_qkv, e_qkv),
        exits=by_owner(gate_exit_grad, up_exit_grad, down_entry_grad),
    )
    g_en_qkv = (select_own * total[:, width:]).astype(BF16)
    g_one = total[:, :width] + dot_t(g_en_qkv, qkv_in)
    in_low = (g_mid + norm_back(inputs, gain_one, g_one)).astype(BF16)
    (g_en_qkv_all,) = gather_tokens(10, g_en_qkv)
    rows_first = entry_grads([(n1, g_en_qkv_all)], n_s, n_c, s)

    attn_grads, rows, input_grad = collect(
        11,
        by_owner(qkv_exit_grad, attn_entry_grad),
        jnp.concatenate([rows_first, rows_mid], axis=2),
        in_low,
    )

    def join(grads, first, count):
        part = grads[:, :, first : first + count]
        return part.transpose(1, 0, 2).reshape(per, n_s * count)

    def join_kv(first):
        part = attn_grads[:, :, first : first + k_cols]
        copies = n_s * kv_take // kv_here
        part = part.reshape(n_s // copies, copies, per, k_cols).sum(axis=1)
        return part.transpose(1, 0, 2).reshape(per, kv_here * HD)

    qkv_eg, gate_eg, up_eg, down_xg, attn_xg = (
        rows[:, i * ranks : (i + 1) * ranks] for i in range(5)
    )
    return (
        as_output(layer_out),
        as_output(input_grad),
        qkv_eg,
        join(attn_grads, 0, q_cols),
        join_kv(q_cols),
        join_kv(q_cols + k_cols),
        join(attn_grads, a_cols, q_cols),
        attn_xg,
        gate_eg,
        join(ffn_grads, 0, f_cols),
        up_eg,
        join(ffn_grads, f_cols, f_cols),
        join(ffn_grads, 2 * f_cols, f_cols),
        down_xg,
    )


def solution(mesh):
    in_specs = (
        P("shard", "context", None),
        P("shard", "context", None),
        P("shard"),
        P("shard"),
        P(),
        P(),
        P(("shard", "context"), "tensor"),
        P(("shard", "context"), "tensor"),
        P(("shard", "context"), "tensor"),
        P(("shard", "context"), "tensor"),
        P(("shard", "context"), "tensor"),
        P(("shard", "context"), "tensor"),
        P(("shard", "context"), "tensor"),
        P(("shard", "context"), None),
        P(("shard", "context"), "tensor"),
        P(("shard", "context"), "tensor"),
        P(("shard", "context"), "tensor"),
        P(("shard", "context"), "tensor"),
        P(("shard", "context"), None),
        P(("shard", "context"), None),
        P(("shard", "context"), "tensor"),
        P(("shard", "context"), None),
        P(("shard", "context"), "tensor"),
        P(("shard", "context"), "tensor"),
        P(("shard", "context"), None),
    )
    out_specs = (
        P("shard", "context", None),
        P("shard", "context", None),
        P(("shard", "context"), None),
        P(("shard", "context"), "tensor"),
        P(("shard", "context"), "tensor"),
        P(("shard", "context"), "tensor"),
        P(("shard", "context"), "tensor"),
        P(("shard", "context"), None),
        P(("shard", "context"), None),
        P(("shard", "context"), "tensor"),
        P(("shard", "context"), None),
        P(("shard", "context"), "tensor"),
        P(("shard", "context"), "tensor"),
        P(("shard", "context"), None),
    )
    return jax.shard_map(shards, mesh=mesh, in_specs=in_specs, out_specs=out_specs, check_vma=False)
```

```python
import functools
import math

import jax
import jax.numpy as jnp
from jax import lax
from jax.experimental import pallas as pl
from jax.experimental.pallas import tpu as pltpu
from jax.sharding import PartitionSpec as P


SHARD, CONTEXT, TENSOR = "shard", "context", "tensor"
HD = 128
RANK = 16
EPSILON = 1e-05
ROPE_BASE = 1000000.0
MASKED = -1e30
F32 = jnp.float32
BF16 = jnp.bfloat16
MESH = pl.DeviceIdType.MESH


def dot(left, right):
    return jnp.dot(left, right, preferred_element_type=F32)


def dot_t(left, right):
    return lax.dot_general(left, right, (((1,), (1,)), ((), ())), preferred_element_type=F32)


def token_sum(left, right):
    return lax.dot_general(left, right, (((0,), (0,)), ((), ())), preferred_element_type=F32)


def rms_scale(values, gain):
    return values * lax.rsqrt(jnp.mean(values * values, axis=-1, keepdims=True) + EPSILON) * gain


def norm_back(values, gain, grad):
    r = lax.rsqrt(jnp.mean(values * values, axis=-1, keepdims=True) + EPSILON)
    scaled = grad * gain
    return r * scaled - values * (r * r * r * jnp.mean(values * scaled, axis=-1, keepdims=True))


def rope(values, cosine, sine):
    return values * cosine + pltpu.roll(values, HD // 2, 1) * sine


def head_tables(positions):
    half = HD // 2
    inverse = ROPE_BASE ** (-2.0 * jnp.arange(half).astype(F32) / HD)
    angles = positions.astype(F32)[:, None] * inverse[None, :]
    cosine, sine = jnp.cos(angles), jnp.sin(angles)
    return jnp.concatenate([cosine, cosine], axis=1), jnp.concatenate([-sine, sine], axis=1)


def masked_scores(query, key, length, first):
    rows, keys = query.shape[0], key.shape[0]
    scores = dot_t(query, key) * (1.0 / math.sqrt(HD))
    at = first + lax.broadcasted_iota(jnp.int32, (rows, keys), 0)
    to = lax.broadcasted_iota(jnp.int32, (rows, keys), 1)
    return jnp.where((to <= at) & (to < length), scores, MASKED)


def attend_kernel(heads, kv_heads, tile, lengths, qkv_ref, cos_ref, sin_ref, att_ref, low_ref, lse_ref):
    length = lengths[pl.program_id(0)]
    full_len = qkv_ref.shape[0]
    for h in range(heads + kv_heads):
        cols = slice(h * HD, (h + 1) * HD)
        low_ref[:, cols] = rope(qkv_ref[:, cols], cos_ref[...], sin_ref[...]).astype(BF16)
    first_value = (heads + kv_heads) * HD
    low_ref[:, first_value:] = qkv_ref[:, first_value:].astype(BF16)
    lse_ref[...] = jnp.zeros_like(lse_ref)
    for first in range(0, full_len, tile):
        rows, keys = slice(first, first + tile), slice(0, first + tile)
        for h in range(heads):
            kv = h * kv_heads // heads
            key = low_ref[keys, (heads + kv) * HD : (heads + kv + 1) * HD]
            value = low_ref[keys, first_value + kv * HD : first_value + (kv + 1) * HD]
            scores = masked_scores(low_ref[rows, h * HD : (h + 1) * HD], key, length, first)
            largest = jnp.max(scores, axis=1, keepdims=True)
            exponent = jnp.exp(scores - largest)
            total = jnp.sum(exponent, axis=1, keepdims=True)
            probs = (exponent / total).astype(BF16)
            att_ref[rows, h * HD : (h + 1) * HD] = dot(probs, value).astype(BF16)
            lse_ref[rows, h : h + 1] = largest + jnp.log(total)


def attend_back_kernel(
    heads, kv_heads, tile, lengths, low_ref, lse_ref, g_ref, cos_ref, sin_ref, out_ref, k_acc, v_acc
):
    length = lengths[pl.program_id(0)]
    full_len = low_ref.shape[0]
    first_value = (heads + kv_heads) * HD
    scale = 1.0 / math.sqrt(HD)
    k_acc[...] = jnp.zeros_like(k_acc)
    v_acc[...] = jnp.zeros_like(v_acc)
    for first in range(0, full_len, tile):
        rows, keys = slice(first, first + tile), slice(0, first + tile)
        for h in range(heads):
            kv = h * kv_heads // heads
            kv_cols = slice(kv * HD, (kv + 1) * HD)
            key = low_ref[keys, (heads + kv) * HD : (heads + kv + 1) * HD]
            value = low_ref[keys, first_value + kv * HD : first_value + (kv + 1) * HD]
            query = low_ref[rows, h * HD : (h + 1) * HD]
            grad = g_ref[rows, h * HD : (h + 1) * HD]
            probs = jnp.exp(masked_scores(query, key, length, first) - lse_ref[rows, h : h + 1])
            g_probs = dot_t(grad, value)
            centre = jnp.sum(probs * g_probs, axis=1, keepdims=True)
            g_scores = (probs * (g_probs - centre)).astype(BF16)
            g_query = dot(g_scores, key) * scale
            out_ref[rows, h * HD : (h + 1) * HD] = rope(
                g_query, cos_ref[rows, :], -sin_ref[rows, :]
            ).astype(BF16)
            k_acc[keys, kv_cols] += token_sum(g_scores, query)
            v_acc[keys, kv_cols] += token_sum(probs.astype(BF16), grad)
    for kv in range(kv_heads):
        cols = slice(kv * HD, (kv + 1) * HD)
        out_ref[:, (heads + kv) * HD : (heads + kv + 1) * HD] = rope(
            k_acc[:, cols] * scale, cos_ref[...], -sin_ref[...]
        ).astype(BF16)
    out_ref[:, first_value:] = v_acc[...].astype(BF16)


def attention(qkv, lengths, groups, heads, kv_heads, tables):
    tokens, cols = qkv.shape
    full_len = tokens // groups
    tile = min(256, full_len)

    def seq(width):
        return pl.BlockSpec((full_len, width), lambda g, lens: (g, 0))

    table = pl.BlockSpec((full_len, HD), lambda g, lens: (0, 0))
    params = pltpu.CompilerParams(vmem_limit_bytes=56 * 1024 * 1024)
    att, low, lse = pl.pallas_call(
        functools.partial(attend_kernel, heads, kv_heads, tile),
        out_shape=(
            jax.ShapeDtypeStruct((tokens, heads * HD), BF16),
            jax.ShapeDtypeStruct((tokens, cols), BF16),
            jax.ShapeDtypeStruct((tokens, HD), F32),
        ),
        grid_spec=pltpu.PrefetchScalarGridSpec(
            num_scalar_prefetch=1,
            grid=(groups,),
            in_specs=[seq(cols), table, table],
            out_specs=[seq(heads * HD), seq(cols), seq(HD)],
        ),
        compiler_params=params,
        name="attend",
    )(lengths, qkv, *tables)

    def backward(grad):
        return pl.pallas_call(
            functools.partial(attend_back_kernel, heads, kv_heads, tile),
            out_shape=jax.ShapeDtypeStruct((tokens, cols), BF16),
            grid_spec=pltpu.PrefetchScalarGridSpec(
                num_scalar_prefetch=1,
                grid=(groups,),
                in_specs=[seq(cols), seq(HD), seq(heads * HD), table, table],
                out_specs=seq(cols),
                scratch_shapes=[
                    pltpu.VMEM((full_len, kv_heads * HD), F32),
                    pltpu.VMEM((full_len, kv_heads * HD), F32),
                ],
            ),
            compiler_params=params,
            name="attend_back",
        )(lengths, low, lse, grad, *tables)

    return att, backward


def ring_at(i, n):
    upper = i // (n // 2)
    return (1 - upper) * 2 * i + upper * (2 * (n - 1 - i) + 1)


def ring_pos(s, n):
    return (1 - s % 2) * (s // 2) + (s % 2) * (n - 1 - s // 2)


def greet(targets):
    barrier = pltpu.get_barrier_semaphore()
    for target in targets:
        pl.semaphore_signal(barrier, inc=1, device_id=target, device_id_type=MESH)
    pl.semaphore_wait(barrier, len(targets))


def send_to(source, target, send_sem, recv_sem, device):
    return pltpu.make_async_remote_copy(
        source, target, send_sem, recv_sem, device_id=device, device_id_type=MESH
    )


def xor(a, b, n):
    total, bit = 0, 1
    while bit < n:
        total = total + ((a // bit + b // bit) % 2) * bit
        bit *= 2
    return total


def home(q, z, k, n):
    return xor(xor(q, z, n), k * (n // 2), n)


def halves(ref, k):
    length = ref.shape[-2] // 2
    return pl.ds(k * length, length)


def others(n, n_c):
    me = lax.axis_index(SHARD) * n_c + lax.axis_index(CONTEXT)
    peers = []
    for k in range(1, n * n_c):
        i = (me + k) % (n * n_c)
        peers.append({SHARD: i // n_c, CONTEXT: i % n_c})
    return peers


class Exchange:
    def __init__(self, n, n_c, source, target, send_sem, recv_sem, own_sem, same):
        s, c = lax.axis_index(SHARD), lax.axis_index(CONTEXT)
        everyone = n * n_c
        me = s * n_c + c
        self.copies, self.arrivals = [], []
        for k, peer in enumerate(others(n, n_c), 1):
            to = (peer[SHARD],) if same else (peer[SHARD], peer[CONTEXT])
            self.copies.append(
                send_to(source.at[to], target.at[s, c], send_sem.at[k], recv_sem.at[k], peer)
            )
            i = (me + everyone - k) % everyone
            slot = target.at[i // n_c, i % n_c]
            self.arrivals.append(send_to(slot, slot, send_sem.at[k], recv_sem.at[k], peer))
        mine = source.at[s] if same else source.at[s, c]
        self.own = pltpu.make_async_copy(mine, target.at[s, c], own_sem.at[0])

    def start(self):
        for copy in self.copies:
            copy.start()
        self.own.start()

    def finish(self):
        self.own.wait()
        for copy in self.arrivals:
            copy.wait_recv()
        for copy in self.copies:
            copy.wait_send()

    @staticmethod
    def sems(n, n_c):
        dma = pltpu.SemaphoreType.DMA
        return [dma((n * n_c,)), dma((n * n_c,)), dma((1,))]


class Arrive:
    def __init__(self, n, source, middle, target, sems):
        self.s, self.c = lax.axis_index(SHARD), lax.axis_index(CONTEXT)
        self.to = [home(self.s, self.c, k, n) for k in (0, 1)]
        self.first, self.second, self.local = [], [], []
        for k in (0, 1):
            rows = halves(source, k)
            self.first.append(
                send_to(
                    source.at[rows], middle.at[rows], sems.at[0, k], sems.at[1, k],
                    {SHARD: self.to[k]},
                )
            )
            self.second.append(
                send_to(
                    middle.at[rows], target.at[rows], sems.at[2, k], sems.at[3, k],
                    {CONTEXT: self.to[k]},
                )
            )
            self.local.append(
                (
                    pltpu.make_async_copy(source.at[rows], middle.at[rows], sems.at[4, k]),
                    pltpu.make_async_copy(middle.at[rows], target.at[rows], sems.at[5, k]),
                )
            )

    def either(self, stage, k, remote, local):
        own = self.s if stage == 0 else self.c
        pl.when(self.to[k] != own)(remote)
        pl.when(self.to[k] == own)(local)

    def start(self):
        for k in (0, 1):
            self.either(0, k, self.first[k].start, self.local[k][0].start)

    def relay(self):
        for k in (0, 1):
            self.either(0, k, self.first[k].wait_recv, self.local[k][0].wait)
            self.either(1, k, self.second[k].start, self.local[k][1].start)

    def finish(self):
        for k in (0, 1):
            self.either(0, k, self.first[k].wait_send, lambda: None)

            def both(copy=self.second[k]):
                copy.wait_send()
                copy.wait_recv()

            self.either(1, k, both, self.local[k][1].wait)

    @staticmethod
    def scratch(shape):
        return [pltpu.VMEM(shape, BF16), pltpu.SemaphoreType.DMA((6, 2))]


class Depart:
    def __init__(self, n, tokens, source, target, sems):
        self.n, self.tokens, self.staged = n, tokens, source
        s, c, t = (lax.axis_index(name) for name in (SHARD, CONTEXT, TENSOR))
        self.stays, self.away, self.kept, self.passed, self.got = [], [], [], [], []
        for k in (0, 1):
            rows = halves(source, k)
            block = home(s, c, k, n)
            self.stays.append((s == c) & (block == s))
            self.away.append(
                send_to(
                    source.at[rows], target.at[t, rows], sems.at[0, k], sems.at[1, k],
                    {SHARD: c, CONTEXT: block},
                )
            )
            self.kept.append(
                pltpu.make_async_copy(source.at[rows], target.at[t, rows], sems.at[4, k])
            )
            for core, group in ((t, self.passed), (1 - t, self.got)):
                spot = target.at[core, rows]
                group.append(
                    send_to(spot, spot, sems.at[2, k], sems.at[3, k], {TENSOR: 1 - t})
                )

    def start(self):
        n, block = self.n, self.tokens.shape[1] // (self.n * self.n)
        for i in range(n * n):
            at = (i % n * n + i // n) * block
            self.staged[:, at : at + block] = self.tokens[:, i * block : (i + 1) * block]
        for k in (0, 1):
            pl.when(~self.stays[k])(self.away[k].start)
            pl.when(self.stays[k])(self.kept[k].start)

    def finish(self):
        for k in (0, 1):
            pl.when(~self.stays[k])(self.away[k].wait_recv)
            pl.when(self.stays[k])(self.kept[k].wait)
            self.passed[k].start()
        for k in (0, 1):
            self.got[k].wait_recv()
            self.passed[k].wait_send()
            pl.when(~self.stays[k])(self.away[k].wait_send)

    @staticmethod
    def scratch(shape):
        return [pltpu.VMEM(shape, BF16), pltpu.SemaphoreType.DMA((5, 2))]


class TileWork:
    def __init__(self, compute, tile, inputs, weights, outputs):
        self.compute, self.tile = compute, tile
        self.inputs, self.weights, self.outputs = inputs, weights, outputs
        self.count = inputs[0].shape[0] // tile

    def operands(self):
        return list(self.inputs) + [weight for weight, _ in self.weights]

    def out_shape(self):
        rows = self.count * self.tile
        return [jax.ShapeDtypeStruct((rows, cols), dtype) for cols, dtype in self.outputs]

    def scratch(self):
        dma = pltpu.SemaphoreType.DMA
        held = [pltpu.VMEM((w.shape[0], cols), w.dtype) for w, cols in self.weights]
        ins = [pltpu.VMEM((2, self.tile, a.shape[1]), a.dtype) for a in self.inputs]
        outs = [pltpu.VMEM((2, self.tile, cols), dtype) for cols, dtype in self.outputs]
        counts = (len(held), len(ins), len(outs))
        return held + ins + outs + [dma((counts[0],)), dma((counts[1], 2)), dma((counts[2], 2))]

    def bind(self, in_refs, out_refs, scratch):
        n_w, n_i, n_o = len(self.weights), len(self.inputs), len(self.outputs)
        self.in_refs, self.weight_refs, self.out_refs = in_refs[:n_i], in_refs[n_i:], out_refs
        self.held, self.ins = scratch[:n_w], scratch[n_w : n_w + n_i]
        self.outs = scratch[n_w + n_i : n_w + n_i + n_o]
        self.held_sem, self.in_sem, self.out_sem = scratch[n_w + n_i + n_o :]

    def hold(self):
        return [
            pltpu.make_async_copy(
                ref.at[:, pl.ds(0, held.shape[1])], held, self.held_sem.at[i]
            )
            for i, (ref, held) in enumerate(zip(self.weight_refs, self.held))
        ]

    def at(self, i):
        return pl.ds(pl.multiple_of(i * self.tile, self.tile), self.tile)

    def load(self, i, slot):
        return [
            pltpu.make_async_copy(ref.at[self.at(i)], buf.at[slot], self.in_sem.at[a, slot])
            for a, (ref, buf) in enumerate(zip(self.in_refs, self.ins))
        ]

    def store(self, i, slot):
        return [
            pltpu.make_async_copy(buf.at[slot], ref.at[self.at(i)], self.out_sem.at[a, slot])
            for a, (ref, buf) in enumerate(zip(self.out_refs, self.outs))
        ]

    def start(self):
        for copy in self.load(0, 0) + self.hold():
            copy.start()

    def run(self, first, last):
        if first == 0:
            for copy in self.hold():
                copy.wait()

        def step(i, carry):
            slot = i % 2
            for copy in self.load(i, slot):
                copy.wait()

            @pl.when(i + 1 < self.count)
            def _():
                for copy in self.load(i + 1, 1 - slot):
                    copy.start()

            @pl.when(i >= 2)
            def _():
                for copy in self.store(i - 2, slot):
                    copy.wait()

            self.compute(
                [buf.at[slot] for buf in self.ins], self.held, [buf.at[slot] for buf in self.outs]
            )
            for copy in self.store(i, slot):
                copy.start()
            return carry

        lax.fori_loop(first, last, step, 0)

    def finish(self):
        for i in range(max(0, self.count - 2), self.count):
            for copy in self.store(i, i % 2):
                copy.wait()


def ffn_tile(ins, held, outs):
    n2, en_gate, en_up = (ref[...] for ref in ins)
    weight, gate_exit, up_exit = held
    cols = gate_exit.shape[1]
    gate = dot(n2, weight[:, :cols]) + dot(en_gate, gate_exit[...])
    outs[0][...] = gate
    up = dot(n2, weight[:, cols:]) + dot(en_up, up_exit[...])
    outs[1][...] = up
    outs[2][...] = (gate * jax.nn.sigmoid(gate) * up).astype(BF16)


def ffn_back_tile(ins, held, outs):
    g_low, g_en_down, gate_ref, up_ref = ins
    w_down, e_down, w_gu, e_gate, e_up = held
    cols = e_down.shape[1]
    g_hidden = dot(g_low[...], w_down[...]) + dot(g_en_down[...], e_down[...])
    gate, up = gate_ref[...], up_ref[...]
    sig = jax.nn.sigmoid(gate)
    outs[0][:, :cols] = (g_hidden * up * (sig * (1.0 + gate * (1.0 - sig)))).astype(BF16)
    outs[0][:, cols:] = (g_hidden * gate * sig).astype(BF16)
    outs[1][...] = dot_t(outs[0][...], w_gu[...]).astype(BF16)
    side = e_gate.shape[0]
    outs[2][:, :side] = dot_t(outs[0][:, :cols], e_gate[...]).astype(BF16)
    outs[2][:, side:] = dot_t(outs[0][:, cols:], e_up[...]).astype(BF16)


def neighbours(n):
    pos = ring_pos(lax.axis_index(SHARD), n)
    sides = tuple({SHARD: ring_at((pos + step) % n, n)} for step in (1, n - 1))
    return pos, sides, {TENSOR: 1 - lax.axis_index(TENSOR)}


def ring_steps(n):
    half = n // 2
    steps = []
    for d in range(1, half + 1):
        steps += [(0, d, 0), (1, d, 1)]
        if d < half:
            steps += [(0, d, 1), (1, d, 0)]
    return steps


def gather_kernel(n, count, work, *refs):
    n_in, n_out = count, count
    if work is not None:
        n_in, n_out = n_in + len(work.operands()), n_out + len(work.outputs)
    sources, outs = refs[:count], refs[n_in : n_in + count]
    ring_send, ring_recv, pair_send, pair_recv, own_sem = refs[n_in + n_out : n_in + n_out + 5]
    if work is not None:
        work.bind(refs[count:n_in], refs[n_in + count : n_in + n_out], refs[n_in + n_out + 5 :])
    half_len = sources[0].shape[0] // 2
    steps = ring_steps(n)
    t = lax.axis_index(TENSOR)
    pos, sides, partner = neighbours(n)
    greet(sides + (partner,))
    arrays = range(count)

    def rows(k):
        return pl.ds(k * half_len, half_len)

    layer = lax.axis_index(CONTEXT)

    def place(a, core, who, k):
        return outs[a].at[core, home(ring_at(who % n, n), layer, k, n), rows(k)]

    def origin(way, d):
        return pos + (n - d if way == 0 else d)

    def sent(a, way, d, k):
        spot = place(a, t, origin(way, d - 1), k)
        source = sources[a].at[rows(k)] if d == 1 else spot
        at = (a, way, d - 1, k)
        return send_to(source, spot, ring_send.at[at], ring_recv.at[at], sides[way])

    def got(a, way, d, k):
        spot, at = place(a, t, origin(way, d), k), (a, way, d - 1, k)
        return send_to(spot, spot, ring_send.at[at], ring_recv.at[at], sides[way])

    def pair(a, core, way, d, k, source=None):
        spot, at = place(a, core, origin(way, d), k), (a, way, d, k)
        return send_to(
            spot if source is None else source, spot, pair_send.at[at], pair_recv.at[at], partner
        )

    waits = []
    for step in steps:
        if step[1] == 1:
            for a in arrays:
                waits.append(sent(a, *step))
                waits[-1].start()
    own = []
    for a in arrays:
        for k in (0, 1):
            waits.append(pair(a, t, 0, 0, k, sources[a].at[rows(k)]))
            waits[-1].start()
            own.append(
                pltpu.make_async_copy(sources[a].at[rows(k)], place(a, t, pos, k), own_sem.at[a, k])
            )
            own[-1].start()
    done = 0
    if work is not None:
        work.start()
    for number, (way, d, k) in enumerate(steps):
        if work is not None and number % 2 == 0 and done < work.count:
            upto = work.count if number + 2 >= len(steps) - 1 else work.count // 2
            work.run(done, upto)
            done = upto
        for a in arrays:
            got(a, way, d, k).wait_recv()
            if (way, d + 1, k) in steps:
                waits.append(sent(a, way, d + 1, k))
                waits[-1].start()
            waits.append(pair(a, t, way, d, k))
            waits[-1].start()
    for a in arrays:
        for step in [(0, 0, 0), (0, 0, 1)] + steps:
            pair(a, 1 - t, *step).wait_recv()
    for copy in waits:
        copy.wait_send()
    for copy in own:
        copy.wait()
    if work is not None:
        if done < work.count:
            work.run(done, work.count)
        work.finish()


def gather_tokens(call, *values, work=None):
    n, count, half = lax.axis_size(SHARD), len(values), lax.axis_size(SHARD) // 2
    dma = pltpu.SemaphoreType.DMA
    out_shape = [jax.ShapeDtypeStruct((2, n) + v.shape, v.dtype) for v in values]
    scratch = [
        dma((count, 2, half, 2)),
        dma((count, 2, half, 2)),
        dma((count, 2, half + 1, 2)),
        dma((count, 2, half + 1, 2)),
        dma((count, 2)),
    ]
    operands = list(values)
    if work is not None:
        operands += work.operands()
        out_shape += work.out_shape()
        scratch += work.scratch()
    any_space = pl.BlockSpec(memory_space=pl.ANY)
    outs = pl.pallas_call(
        functools.partial(gather_kernel, n, count, work),
        out_shape=out_shape,
        in_specs=[pl.BlockSpec(memory_space=pltpu.VMEM)] * count
        + [any_space] * (len(operands) - count),
        out_specs=[any_space] * len(out_shape),
        scratch_shapes=scratch,
        compiler_params=pltpu.CompilerParams(
            collective_id=call, has_side_effects=True, vmem_limit_bytes=56 * 1024 * 1024
        ),
        cost_estimate=pl.CostEstimate(flops=0, bytes_accessed=100_000_000, transcendentals=0),
    )(*operands)
    full = [out.reshape(2 * n * v.shape[0], v.shape[1]) for out, v in zip(outs, values)]
    return full + list(outs[count:])


def scatter_tokens(call, *values, arrive=None, depart=None, exits=None, work=None):
    n, n_c, count = lax.axis_size(SHARD), lax.axis_size(CONTEXT), len(values)
    cols = sum(v.shape[1] for v in values)
    length = values[0].shape[0] // (2 * n)
    half, half_len = n // 2, length // 2
    steps = ring_steps(n)

    def kernel(*refs):
        refs = list(refs)
        parts = [refs.pop(0) for _ in range(count)]
        arrive_ref = refs.pop(0) if arrive is not None else None
        depart_ref = refs.pop(0) if depart is not None else None
        exits_ref = refs.pop(0) if exits is not None else None
        work_in = [refs.pop(0) for _ in range(len(work.operands()))] if work is not None else []
        out_ref = refs.pop(0)
        arrive_out = refs.pop(0) if arrive is not None else None
        depart_out = refs.pop(0) if depart is not None else None
        exits_out = refs.pop(0) if exits is not None else None
        work_out = [refs.pop(0) for _ in range(len(work.outputs))] if work is not None else []
        mine, other, inbox = [refs.pop(0) for _ in range(3)]
        ring_send, ring_recv, pair_send, pair_recv, load_sem = [refs.pop(0) for _ in range(5)]
        t = lax.axis_index(TENSOR)
        layer = lax.axis_index(CONTEXT)
        pos, sides, partner = neighbours(n)
        jobs = []
        if arrive is not None:
            jobs.append(Arrive(n, arrive_ref, refs.pop(0), arrive_out, refs.pop(0)))
        if depart is not None:
            jobs.append(Depart(n, depart_ref, refs.pop(0), depart_out, refs.pop(0)))
        if exits is not None:
            exits_in = refs.pop(0)
            jobs.append(
                Exchange(n, n_c, exits_ref, exits_in, *(refs.pop(0) for _ in range(3)), False)
            )
        cuts = [0, 0, 0, 0]
        if work is not None:
            work.bind(work_in, work_out, refs)
            cuts = [work.count * part // 8 for part in (1, 2, 5, 8)]
        greet((others(n, n_c) if jobs else list(sides)) + [partner])
        order = [half]
        for d in range(half - 1, 0, -1):
            order += [d, n - d]
        order.append(0)

        def rows(k):
            return pl.ds(k * half_len, half_len)

        swaps, loads = {}, {}
        for d in order:
            who = ring_at((pos + d) % n, n)
            swaps[d], loads[d], first = [], [], 0
            for a, part in enumerate(parts):
                cols_a = pl.ds(first, part.shape[-1])
                first += part.shape[-1]
                for k in (0, 1):
                    at = (a, d, k)
                    block = home(who, layer, k, n)
                    loads[d].append(
                        pltpu.make_async_copy(
                            part.at[t, block, rows(k)], mine.at[d, rows(k), cols_a], load_sem.at[at]
                        )
                    )
                    swaps[d].append(
                        send_to(
                            part.at[1 - t, block, rows(k)], other.at[d, rows(k), cols_a],
                            pair_send.at[at], pair_recv.at[at], partner,
                        )
                    )
                    swaps[d][-1].start()
                    loads[d][-1].start()
        for job in jobs:
            job.start()
        if work is not None:
            work.start()

        def advance(part):
            first, last = (0, *cuts)[part], cuts[part]
            if last > first:
                work.run(first, last)

        def ready(d):
            for copy in loads[d]:
                copy.wait()
            for copy in swaps[d]:
                copy.wait_recv()

        def chip_sum(d, k):
            return mine[d, rows(k), :].astype(F32) + other[d, rows(k), :].astype(F32)

        def ring(way, d, k):
            at = (way, d - 1, k)
            index = d if way == 0 else n - d
            return send_to(
                mine.at[index, rows(k)], inbox.at[way, d - 1, rows(k)], ring_send.at[at],
                ring_recv.at[at], sides[way],
            )

        def send(way, d, k, total):
            mine[d if way == 0 else n - d, rows(k), :] = total.astype(BF16)
            ring(way, d, k).start()

        def taken(way, d, k):
            ring(way, d, k).wait_recv()
            return inbox[way, d - 1, rows(k), :].astype(F32)

        advance(0)
        ready(half)
        send(0, half, 0, chip_sum(half, 0))
        send(1, half, 1, chip_sum(half, 1))
        advance(1)
        for d in range(half - 1, 0, -1):
            for way, index in ((0, d), (1, n - d)):
                ready(index)
                k = 1 - way
                total = chip_sum(index, k)
                if (way, d + 1, k) in steps:
                    total = total + taken(way, d + 1, k)
                send(way, d, k, total)
            if d == half - 1:
                advance(2)
            for way, index in ((0, d), (1, n - d)):
                send(way, d, way, chip_sum(index, way) + taken(way, d + 1, way))
        advance(3)
        if arrive is not None:
            jobs[0].relay()
        ready(0)
        for k in (0, 1):
            out_ref[rows(k), :] = chip_sum(0, k)
        for way, k in ((0, 1), (1, 0), (0, 0), (1, 1)):
            out_ref[rows(k), :] += taken(way, 1, k)
        for step in steps:
            ring(*step).wait_send()
        for d in order:
            for copy in swaps[d]:
                copy.wait_send()
        for job in jobs:
            job.finish()
        if exits is not None:
            add_layers(exits_in, exits_out)
        if work is not None:
            work.finish()

    dma = pltpu.SemaphoreType.DMA
    any_space, vmem = pl.BlockSpec(memory_space=pl.ANY), pl.BlockSpec(memory_space=pltpu.VMEM)
    operands = [v.astype(BF16).reshape(2, n, length, v.shape[1]) for v in values]
    in_specs, out_specs = [any_space] * count, [vmem]
    out_shape = [jax.ShapeDtypeStruct((length, cols), F32)]
    scratch = [
        pltpu.VMEM((n, length, cols), BF16),
        pltpu.VMEM((n, length, cols), BF16),
        pltpu.VMEM((2, half, length, cols), BF16),
        dma((2, half, 2)),
        dma((2, half, 2)),
        dma((count, n, 2)),
        dma((count, n, 2)),
        dma((count, n, 2)),
    ]
    if arrive is not None:
        operands.append(arrive)
        in_specs.append(vmem)
        out_specs.append(any_space)
        out_shape.append(jax.ShapeDtypeStruct(arrive.shape, BF16))
        scratch += Arrive.scratch(arrive.shape)
    if depart is not None:
        operands.append(depart)
        in_specs.append(vmem)
        out_specs.append(any_space)
        out_shape.append(jax.ShapeDtypeStruct((2,) + depart.shape, BF16))
        scratch += Depart.scratch(depart.shape)
    if exits is not None:
        operands.append(exits)
        in_specs.append(vmem)
        out_specs.append(vmem)
        out_shape.append(jax.ShapeDtypeStruct((n,) + exits.shape[2:], F32))
        scratch += [pltpu.VMEM(exits.shape, BF16)] + Exchange.sems(n, n_c)
    if work is not None:
        operands += work.operands()
        in_specs += [any_space] * len(work.operands())
        out_specs += [any_space] * len(work.outputs)
        out_shape += work.out_shape()
        scratch += work.scratch()
    return pl.pallas_call(
        kernel,
        out_shape=out_shape,
        in_specs=in_specs,
        out_specs=out_specs,
        scratch_shapes=scratch,
        compiler_params=pltpu.CompilerParams(
            collective_id=call, has_side_effects=True, vmem_limit_bytes=60 * 1024 * 1024
        ),
        cost_estimate=pl.CostEstimate(flops=0, bytes_accessed=100_000_000, transcendentals=0),
    )(*operands)


def add_layers(inbox, out_ref):
    for q in range(inbox.shape[0]):
        total = inbox[q, 0].astype(F32)
        for i in range(1, inbox.shape[1]):
            total = total + inbox[q, i].astype(F32)
        out_ref[q] = total


def spread(call, sources, items, widths, wide, tokens=None):
    n, n_c = lax.axis_size(SHARD), lax.axis_size(CONTEXT)
    n_in, n_out = len(sources), len(widths)
    rows = sources[0].shape[0]

    def kernel(*refs):
        refs = list(refs)
        ins = [refs.pop(0) for _ in range(n_in)]
        wide_ref = refs.pop(0)
        tokens_ref = refs.pop(0) if tokens is not None else None
        outs = [refs.pop(0) for _ in range(n_out)]
        wide_out = refs.pop(0)
        tokens_out = refs.pop(0) if tokens is not None else None
        send_sem, recv_sem, own_sem = refs.pop(0), refs.pop(0), refs.pop(0)
        s = lax.axis_index(SHARD)
        exchange = Exchange(n, n_c, wide_ref, wide_out, *(refs.pop(0) for _ in range(3)), True)
        arrive = None
        if tokens is not None:
            arrive = Arrive(n, tokens_ref, refs.pop(0), tokens_out, refs.pop(0))
        bounce = refs
        greet(others(n, n_c))

        def piece(item, q):
            source, _, _, width, kind, heads = items[item]
            if kind == "split":
                first = pl.multiple_of(q * width, HD)
            elif kind == "kv":
                first = pl.multiple_of((q * heads // n) * HD, HD)
            else:
                first = 0
            return ins[source].at[:, pl.ds(first, width)]

        def spot(item, q):
            _, out, first, width, _, _ = items[item]
            return outs[out].at[q, :, pl.ds(first, width)]

        if arrive is not None:
            arrive.start()
        waits, own, arrivals = [], [], []
        for item in range(len(items)):
            for k in range(1, n):
                q = (s + k) % n
                at = (item, k)
                copy = send_to(
                    piece(item, q), spot(item, s), send_sem.at[at], recv_sem.at[at], {SHARD: q}
                )
                copy.start()
                waits.append(copy)
                q = (s + n - k) % n
                arrivals.append(
                    send_to(
                        spot(item, q), spot(item, q), send_sem.at[at], recv_sem.at[at], {SHARD: q}
                    )
                )
            copy = pltpu.make_async_copy(piece(item, s), bounce[item], own_sem.at[item, 0])
            copy.start()
            own.append(copy)
        exchange.start()
        stored = []
        for item in range(len(items)):
            own[item].wait()
            copy = pltpu.make_async_copy(bounce[item], spot(item, s), own_sem.at[item, 1])
            copy.start()
            stored.append(copy)
        if arrive is not None:
            arrive.relay()
        for copy in stored:
            copy.wait()
        exchange.finish()
        for copy in arrivals:
            copy.wait_recv()
        for copy in waits:
            copy.wait_send()
        if arrive is not None:
            arrive.finish()

    dma = pltpu.SemaphoreType.DMA
    any_space, vmem = pl.BlockSpec(memory_space=pl.ANY), pl.BlockSpec(memory_space=pltpu.VMEM)
    scratch = [dma((len(items), n)), dma((len(items), n)), dma((len(items), 2))]
    scratch += Exchange.sems(n, n_c)
    out_shape = [jax.ShapeDtypeStruct((n, rows, w), BF16) for w in widths]
    out_shape.append(jax.ShapeDtypeStruct((n, n_c) + wide.shape[1:], BF16))
    operands = list(sources) + [wide]
    if tokens is not None:
        operands.append(tokens)
        scratch += Arrive.scratch(tokens.shape)
        out_shape.append(jax.ShapeDtypeStruct(tokens.shape, BF16))
    scratch += [pltpu.VMEM((rows, item[3]), BF16) for item in items]
    return pl.pallas_call(
        kernel,
        out_shape=out_shape,
        in_specs=[any_space] * n_in + [vmem] * (len(operands) - n_in),
        out_specs=[any_space] * len(out_shape),
        scratch_shapes=scratch,
        compiler_params=pltpu.CompilerParams(collective_id=call, has_side_effects=True),
        cost_estimate=pl.CostEstimate(flops=0, bytes_accessed=40_000_000, transcendentals=0),
    )(*operands)


def collect(call, exits, plane, rows, depart):
    n, n_c = exits.shape[:2]

    def kernel(
        exits_ref, plane_ref, rows_ref, depart_ref, exits_out, plane_out, rows_out, depart_out,
        exits_in, rows_in, row_box, stage, *sems,
    ):
        s = lax.axis_index(SHARD)
        leave = Depart(n, depart_ref, stage, depart_out, sems[0])
        exchange = Exchange(n, n_c, exits_ref, exits_in, *sems[1:4], False)
        row_exchange = Exchange(n, n_c, rows_ref, rows_in, *sems[4:7], False)
        partner = {TENSOR: 1 - lax.axis_index(TENSOR)}
        greet(others(n, n_c) + [partner])
        row_exchange.start()
        leave.start()
        waits, arrivals = [], []

        def move(source, target, via, sem, to):
            waits.append(send_to(source, target, sem[0], sem[1], to))
            waits[-1].start()
            arrivals.append(send_to(via, via, sem[0], sem[1], to))

        for k in range(1, n):
            to, via = (s + k) % n, (s + n - k) % n
            sem = (sems[7].at[0, k], sems[7].at[1, k])
            move(plane_ref.at[to], plane_out.at[s], plane_out.at[via], sem, {SHARD: to})
        exchange.start()
        kept = pltpu.make_async_copy(plane_ref.at[s], plane_out.at[s], sems[7].at[0, 0])
        kept.start()
        row_exchange.finish()
        total = jnp.zeros(rows_out.shape, F32)
        for q in range(n):
            for i in range(n_c):
                total = total + rows_in[q, i].astype(F32)
        row_box[0] = total
        pair = send_to(row_box.at[0], row_box.at[1], sems[8].at[0], sems[8].at[1], partner)
        pair.start()
        kept.wait()
        for copy in arrivals:
            copy.wait_recv()
        exchange.finish()
        add_layers(exits_in, exits_out)
        leave.finish()
        pair.wait_recv()
        rows_out[...] = row_box[0] + row_box[1]
        pair.wait_send()
        for copy in waits:
            copy.wait_send()

    vmem = pl.BlockSpec(memory_space=pltpu.VMEM)
    return pl.pallas_call(
        kernel,
        out_shape=(
            jax.ShapeDtypeStruct((n,) + exits.shape[2:], F32),
            jax.ShapeDtypeStruct(plane.shape, BF16),
            jax.ShapeDtypeStruct(rows.shape[2:], F32),
            jax.ShapeDtypeStruct((2,) + depart.shape, BF16),
        ),
        in_specs=[vmem] * 4,
        out_specs=(vmem, vmem, vmem, pl.BlockSpec(memory_space=pl.ANY)),
        scratch_shapes=[
            pltpu.VMEM(exits.shape, BF16),
            pltpu.VMEM(rows.shape, BF16),
            pltpu.VMEM((2,) + rows.shape[2:], F32),
            *Depart.scratch(depart.shape),
            *Exchange.sems(n, n_c),
            *Exchange.sems(n, n_c),
            pltpu.SemaphoreType.DMA((2, n)),
            pltpu.SemaphoreType.DMA((2,)),
        ],
        compiler_params=pltpu.CompilerParams(collective_id=call, has_side_effects=True),
        cost_estimate=pl.CostEstimate(flops=0, bytes_accessed=60_000_000, transcendentals=0),
    )(exits, plane, rows, depart)


def entry_grads(pairs, n_s, n_c, s):
    tokens, width = pairs[0][0].shape
    block = width // (n_s * n_c)
    if block % HD:
        parts = []
        for acts, side in pairs:
            mine = lax.dynamic_index_in_dim(
                acts.reshape(tokens, n_c, n_s, block), s, 2, keepdims=False
            )
            parts.append(token_sum(mine.reshape(tokens, n_c * block), side))
        return jnp.concatenate(parts, axis=1).astype(BF16).reshape(n_c, block, -1)
    count = len(pairs)
    total = sum(side.shape[1] for _, side in pairs)

    def kernel(_, *refs):
        first = 0
        for a in range(count):
            cols = slice(first, first + refs[count + a].shape[1])
            first = cols.stop
            refs[-1][0, :, cols] = token_sum(refs[a][...], refs[count + a][...]).astype(BF16)

    return pl.pallas_call(
        kernel,
        out_shape=jax.ShapeDtypeStruct((n_c, block, total), BF16),
        grid_spec=pltpu.PrefetchScalarGridSpec(
            num_scalar_prefetch=1,
            grid=(n_c,),
            in_specs=[pl.BlockSpec((tokens, block), lambda i, at: (0, i * n_s + at[0]))] * count
            + [pl.BlockSpec(side.shape, lambda i, at: (0, 0)) for _, side in pairs],
            out_specs=pl.BlockSpec((1, block, total), lambda i, at: (i, 0, 0)),
        ),
        name="entry_grads",
    )(s.reshape(1).astype(jnp.int32), *(a for a, _ in pairs), *(b for _, b in pairs))


def shards(
    hidden_in,
    cotangent,
    seq_lengths,
    adapter_ids,
    attn_gain,
    ffn_gain,
    query_weight,
    key_weight,
    value_weight,
    output_weight,
    gate_weight,
    up_weight,
    down_weight,
    qkv_entry,
    query_exit,
    key_exit,
    value_exit,
    attn_entry,
    attn_exit,
    gate_entry,
    gate_exit,
    up_entry,
    up_exit,
    down_entry,
    down_exit,
):
    n_s, n_c = lax.axis_size(SHARD), lax.axis_size(CONTEXT)
    s, t = lax.axis_index(SHARD), lax.axis_index(TENSOR)
    groups, local_len, width = hidden_in.shape
    block = width // (n_s * n_c)
    full_len = local_len * n_c
    tokens = groups * full_len
    ranks = qkv_entry.shape[1]
    swap = [(a * n_c + b, b * n_c + a) for a in range(n_s) for b in range(n_c)]

    def own_tokens(values):
        own = lax.dynamic_index_in_dim(values, t, 0, keepdims=False)
        own = own.reshape(local_len, n_s, n_c, block).transpose(0, 2, 1, 3)
        return own.reshape(local_len, width)

    def features(vector):
        return vector.reshape(n_s, n_c, block).transpose(1, 0, 2).reshape(width).astype(F32)

    q_cols = query_weight.shape[1] // n_s
    f_cols = gate_weight.shape[1] // n_s
    kv_here = key_weight.shape[1] // HD
    kv_take = max(1, kv_here // n_s)
    k_cols = kv_take * HD
    heads = q_cols // HD
    a_cols = q_cols + 2 * k_cols

    def split(weights):
        rows, cols = weights.shape
        return weights.reshape(rows, n_s, cols // n_s).transpose(1, 0, 2)

    def split_kv(weights):
        first = [q * kv_here // n_s * HD for q in range(n_s)]
        return jnp.stack([weights[:, at : at + k_cols] for at in first])

    exits_a = jnp.concatenate(
        [split(query_exit), split_kv(key_exit), split_kv(value_exit), split(attn_entry)], axis=2
    )
    exits_f = jnp.concatenate([split(gate_exit), split(up_exit), split(down_entry)], axis=2)
    entry_a = jnp.where(t == 0, qkv_entry, attn_exit)
    entry_f = jnp.where(t == 0, gate_entry, up_entry)
    attn_pack, exits_a = spread(
        0,
        [query_weight, key_weight, value_weight, output_weight, entry_a],
        [
            (0, 0, 0, q_cols, "split", 0),
            (1, 0, q_cols, k_cols, "kv", kv_here),
            (2, 0, q_cols + k_cols, k_cols, "kv", kv_here),
            (3, 0, a_cols, q_cols, "split", 0),
            (4, 0, a_cols + q_cols, ranks, "same", 0),
        ],
        [a_cols + q_cols + ranks],
        exits_a,
    )
    gu_pack, down_pack, exits_f, x_low = spread(
        1,
        [gate_weight, up_weight, entry_f, down_exit, down_weight],
        [
            (0, 0, 0, f_cols, "split", 0),
            (1, 0, f_cols, f_cols, "split", 0),
            (2, 0, 2 * f_cols, ranks, "same", 0),
            (3, 0, 2 * f_cols + ranks, ranks, "same", 0),
            (4, 1, 0, f_cols, "split", 0),
        ],
        [2 * f_cols + 2 * ranks, f_cols],
        exits_f,
        own_tokens(hidden_in),
    )

    def along(pack):
        return lax.all_gather(pack, CONTEXT, axis=0).reshape(width, -1)

    def both_cores(mine):
        theirs = lax.ppermute(mine, TENSOR, [(0, 1), (1, 0)])
        return jnp.where(t == 0, mine, theirs), jnp.where(t == 0, theirs, mine)

    attn_w = along(attn_pack)
    own_cot, x_low = lax.optimization_barrier((own_tokens(cotangent), x_low))
    part_len = local_len // 2
    cot_halves = []
    for k in (0, 1):
        half = own_cot[k * part_len : (k + 1) * part_len]
        spots = [(a, b, home(a, b, k, n_s)) for a in range(n_s) for b in range(n_c)]
        half = lax.ppermute(
            half, (SHARD, CONTEXT), [(a * n_c + b, to * n_c + b) for a, b, to in spots]
        )
        half = lax.ppermute(
            half, (SHARD, CONTEXT), [(a * n_c + b, a * n_c + to) for a, b, to in spots]
        )
        cot_halves.append(half)
    cot_low = jnp.concatenate(cot_halves, axis=0)
    gu_w = along(gu_pack)
    w_d = along(down_pack)
    exits_a, exits_f = exits_a.reshape(ranks, -1), exits_f.reshape(ranks, -1)
    lengths, ids = lax.ppermute(
        jnp.stack([seq_lengths, adapter_ids]), (SHARD, CONTEXT), swap
    )
    gain_one, gain_two = features(attn_gain), features(ffn_gain)
    layer = lax.axis_index(CONTEXT)
    positions = jnp.concatenate(
        [
            home(s, layer, k, n_s) * local_len + k * part_len + jnp.arange(part_len)
            for k in (0, 1)
        ]
    )
    valid = (positions < lengths[t]).astype(F32)[:, None]
    chosen = (jnp.arange(ranks)[None, :] // RANK == ids[:, None]).astype(F32)
    select_own = chosen[t][None, :]
    select_all = jnp.broadcast_to(chosen[:, None, :], (groups, full_len, ranks)).reshape(
        tokens, ranks
    )
    w_qkv, w_o = attn_w[:, :a_cols], attn_w[:, a_cols : a_cols + q_cols]
    e_qkv, e_o = exits_a[:, :a_cols], exits_a[:, a_cols:]
    qkv_in, attn_out = both_cores(attn_w[:, a_cols + q_cols :])
    gate_in, up_in = both_cores(gu_w[:, 2 * f_cols : 2 * f_cols + ranks])
    down_out = gu_w[:, 2 * f_cols + ranks :]
    e_g, e_u, e_d = (exits_f[:, i * f_cols : (i + 1) * f_cols] for i in range(3))

    inputs = x_low.astype(F32)
    n1_own = rms_scale(inputs, gain_one).astype(BF16)
    (n1,) = gather_tokens(2, n1_own)
    en_qkv = (select_all * dot(n1, qkv_in)).astype(BF16)
    qkv = dot(n1, w_qkv) + dot(en_qkv, e_qkv)
    att, attention_back = attention(
        qkv, lengths, groups, heads, kv_take, head_tables(jnp.arange(full_len))
    )
    (total,) = scatter_tokens(3, dot_t(att, w_o), dot_t(att, e_o))
    en_attn = (select_own * total[:, width:]).astype(BF16)
    mid = inputs + total[:, :width] + dot_t(en_attn, attn_out)

    n2, en_attn_all = gather_tokens(4, rms_scale(mid, gain_two).astype(BF16), en_attn)
    en_gate = (select_all * dot(n2, gate_in)).astype(BF16)
    en_up = (select_all * dot(n2, up_in)).astype(BF16)
    grad_out = valid * cot_low.astype(F32)
    g_low, gate, up, hidden = gather_tokens(
        6,
        grad_out.astype(BF16),
        work=TileWork(
            ffn_tile,
            min(512, tokens // 2),
            [n2, en_gate, en_up],
            [(gu_w, 2 * f_cols), (e_g, f_cols), (e_u, f_cols)],
            [(f_cols, F32), (f_cols, F32), (f_cols, BF16)],
        ),
    )
    g_en_down = (select_all * dot(g_low, down_out)).astype(BF16)
    total, g_gu, part, side = scatter_tokens(
        5,
        dot_t(hidden, w_d),
        dot_t(hidden, e_d),
        work=TileWork(
            ffn_back_tile,
            min(256, tokens // 8),
            [g_low, g_en_down, gate, up],
            [(w_d, f_cols), (e_d, f_cols), (gu_w, 2 * f_cols), (e_g, f_cols), (e_u, f_cols)],
            [(2 * f_cols, BF16), (width, BF16), (2 * ranks, BF16)],
        ),
    )
    en_down = (select_own * total[:, width:]).astype(BF16)
    layer_sum = mid + total[:, :width] + dot_t(en_down, down_out)
    out_low = (valid * layer_sum).astype(BF16)

    down_entry_grad = token_sum(g_en_down, hidden)
    gate_exit_grad = token_sum(en_gate, g_gu[:, :f_cols])
    up_exit_grad = token_sum(en_up, g_gu[:, f_cols:])
    per = ranks // (n_s * n_c)
    ffn_grads = jnp.concatenate([gate_exit_grad, up_exit_grad, down_entry_grad], axis=1)
    ffn_grads = ffn_grads.reshape(n_s, n_c, per, -1).transpose(1, 0, 2, 3)
    ffn_grads = lax.psum_scatter(
        ffn_grads.reshape(ranks, -1), CONTEXT, scatter_dimension=0, tiled=True
    )
    total, layer_out = scatter_tokens(
        7,
        part,
        side,
        depart=out_low,
    )
    g_en_gu = (
        jnp.concatenate([select_own, select_own], axis=1) * total[:, width:]
    ).astype(BF16)
    g_two = (
        total[:, :width]
        + dot_t(g_en_gu[:, :ranks], gate_in)
        + dot_t(g_en_gu[:, ranks:], up_in)
    )
    g_mid = grad_out + norm_back(mid, gain_two, g_two)
    g_mid_all, side = gather_tokens(
        8, g_mid.astype(BF16), jnp.concatenate([g_en_gu, en_down], axis=1)
    )
    rows_mid = entry_grads(
        [(n2, side[:, : 2 * ranks]), (g_low, side[:, 2 * ranks :]), (g_mid_all, en_attn_all)],
        n_s,
        n_c,
        s,
    )

    rows_mid, g_mid_all = lax.optimization_barrier((rows_mid, g_mid_all))
    rows_mid = lax.psum_scatter(rows_mid.astype(F32), CONTEXT, scatter_dimension=0)

    g_en_attn = (select_all * dot(g_mid_all, attn_out)).astype(BF16)
    attn_entry_grad = token_sum(g_en_attn, att)
    g_att = (dot(g_mid_all, w_o) + dot(g_en_attn, e_o)).astype(BF16)
    g_qkv = attention_back(g_att)
    qkv_exit_grad = token_sum(en_qkv, g_qkv)
    (total,) = scatter_tokens(
        9,
        dot_t(g_qkv, w_qkv),
        dot_t(g_qkv, e_qkv),
    )
    g_en_qkv = (select_own * total[:, width:]).astype(BF16)
    g_one = total[:, :width] + dot_t(g_en_qkv, qkv_in)
    in_low = (g_mid + norm_back(inputs, gain_one, g_one)).astype(BF16)
    rows_first = token_sum(n1_own, g_en_qkv).astype(BF16)
    rows_first = rows_first.reshape(n_c, n_s, block, ranks).transpose(1, 0, 2, 3)

    attn_grads, ffn_grads, rows_first, input_grad = collect(
        11,
        jnp.concatenate([qkv_exit_grad, attn_entry_grad], axis=1)
        .astype(BF16)
        .reshape(n_s, n_c, per, -1),
        ffn_grads.astype(BF16).reshape(n_s, per, -1),
        rows_first,
        in_low,
    )
    ffn_grads = ffn_grads.astype(F32)
    rows = jnp.concatenate([rows_first, rows_mid], axis=1)

    def join(grads, first, count):
        part = grads[:, :, first : first + count]
        return part.transpose(1, 0, 2).reshape(per, n_s * count)

    def join_kv(first):
        part = attn_grads[:, :, first : first + k_cols]
        copies = n_s * kv_take // kv_here
        part = part.reshape(n_s // copies, copies, per, k_cols).sum(axis=1)
        return part.transpose(1, 0, 2).reshape(per, kv_here * HD)

    qkv_eg, gate_eg, up_eg, down_xg, attn_xg = (
        rows[:, i * ranks : (i + 1) * ranks] for i in range(5)
    )
    return (
        layer_out,
        input_grad,
        qkv_eg,
        join(attn_grads, 0, q_cols),
        join_kv(q_cols),
        join_kv(q_cols + k_cols),
        join(attn_grads, a_cols, q_cols),
        attn_xg,
        gate_eg,
        join(ffn_grads, 0, f_cols),
        up_eg,
        join(ffn_grads, f_cols, f_cols),
        join(ffn_grads, 2 * f_cols, f_cols),
        down_xg,
    )


def solution(mesh):
    in_specs = (
        P(SHARD, CONTEXT, None),
        P(SHARD, CONTEXT, None),
        P(SHARD),
        P(SHARD),
        P(),
        P(),
        P((SHARD, CONTEXT), TENSOR),
        P((SHARD, CONTEXT), TENSOR),
        P((SHARD, CONTEXT), TENSOR),
        P((SHARD, CONTEXT), TENSOR),
        P((SHARD, CONTEXT), TENSOR),
        P((SHARD, CONTEXT), TENSOR),
        P((SHARD, CONTEXT), TENSOR),
        P((SHARD, CONTEXT), None),
        P((SHARD, CONTEXT), TENSOR),
        P((SHARD, CONTEXT), TENSOR),
        P((SHARD, CONTEXT), TENSOR),
        P((SHARD, CONTEXT), TENSOR),
        P((SHARD, CONTEXT), None),
        P((SHARD, CONTEXT), None),
        P((SHARD, CONTEXT), TENSOR),
        P((SHARD, CONTEXT), None),
        P((SHARD, CONTEXT), TENSOR),
        P((SHARD, CONTEXT), TENSOR),
        P((SHARD, CONTEXT), None),
    )
    out_specs = (
        P(SHARD, CONTEXT, None),
        P(SHARD, CONTEXT, None),
        P((SHARD, CONTEXT), None),
        P((SHARD, CONTEXT), TENSOR),
        P((SHARD, CONTEXT), TENSOR),
        P((SHARD, CONTEXT), TENSOR),
        P((SHARD, CONTEXT), TENSOR),
        P((SHARD, CONTEXT), None),
        P((SHARD, CONTEXT), None),
        P((SHARD, CONTEXT), TENSOR),
        P((SHARD, CONTEXT), None),
        P((SHARD, CONTEXT), TENSOR),
        P((SHARD, CONTEXT), TENSOR),
        P((SHARD, CONTEXT), None),
    )

    return jax.shard_map(shards, mesh=mesh, in_specs=in_specs, out_specs=out_specs, check_vma=False)
```
